32 devices in a mesh: grp: 2 (over core), tab: 16 (over z, y, x).
Axes of the slice: x: 2, y: 2, z: 4, core: 2. Of those that a mesh axis runs over, the one named last changes fastest.
Arguments:
- sample_ids: int32 [4, 1024, 1024], P(None, ('grp', 'tab')), may hold values from 0 to 1535
- id_weights: bfloat16 [4, 1024, 1024], P(None, ('grp', 'tab')), may hold values from 0.25 to 2
- dense_features: bfloat16 [4, 1024, 128], P(None, ('grp', 'tab')), may hold values from -6 to 6
- click_labels: int32 [4, 1024], P(None, ('grp', 'tab')), may hold values 0 or 1
- table_shards: bfloat16 [128, 1536, 128], P('tab'), may hold values from -1.1953125 to 1.1953125
- slot_table: int32 [128], replicated, may hold values from 0 to 127, each once
- top_weight: bfloat16 [128, 1024], replicated, may hold values from -0.5 to 0.5
- top_bias: float32 [1024], replicated, may hold values from -3 to 3
- out_weight: bfloat16 [1024], replicated, may hold values from -0.1875 to 0.1875
Outputs:
- logits: float32 [4, 1024], P(None, ('grp', 'tab'))
- grad_top: float32 [128, 1024], replicated
- grad_bias: float32 [1024], replicated
The draws below stay inside these ranges and needn't reach their ends.
Inputs may be any that keep to these rules, and one draw needn't show every extreme that they name: `slot_table`: a permutation: each table stands in exactly one slot.
All inputs are finite; a program needn't handle non-finite values. No bound on the sum of `click_labels` on one device may be relied on, other than what follows from the above.
Results may differ from the reference program's by a relative error of at most 0.0056.
Values may be sent and summed in bfloat16 or wider, within the bound.
A program may use at most 128 MiB of HBM per device.

```python
import math
import jax
import jax.numpy as jnp
import numpy as np
from jax import lax

DIM = 128
VOCAB = 1536
HIDDEN_SIZE = 1024
HOTS = 8
MB = 4
TABLES = 128
BATCH = 1024


def place_ends(entries, key, smallest, largest):
    dims = entries.shape
    spot = [jax.random.randint(jax.random.fold_in(key, axis), (), 0, dims[axis]) for axis in range(len(dims))]
    entries = entries.at[tuple(spot)].set(smallest)
    longest = dims.index(max(dims))
    spot[longest] = (spot[longest] + 1) % dims[longest]
    return entries.at[tuple(spot)].set(largest)


def shard_levels(stream_key, dims, cuts, low, high):
    level, own = 1.0, jax.random.fold_in(stream_key, 6)
    for dim, blocks in cuts:
        steps = jnp.exp(jax.random.uniform(jax.random.fold_in(own, dim), (blocks,), jnp.float32, low / len(cuts), high / len(cuts)))
        level = level * jnp.repeat(steps, dims[dim] // blocks).reshape([-1 if axis == dim else 1 for axis in range(len(dims))])
    return level


def cumulative_ranks(count, lean):
    weights = [(1 << 20) // math.isqrt(standing ** lean) + 1 for standing in range(1, count + 1)]
    spread = 1 + sum(weights) // (1 << 30)
    return np.cumsum(np.array([max(1, weight // spread) for weight in weights]))


def skewed_ids(own_key, shape, number_of, skew):
    table = cumulative_ranks(number_of, skew)
    pick = jax.random.randint(jax.random.fold_in(own_key, 1), shape, 0, int(table[number_of - 1]))
    standing = jnp.searchsorted(jnp.asarray(table, jnp.int32), pick, side="right")
    return jax.random.permutation(jax.random.fold_in(own_key, 2), number_of)[standing].astype(jnp.int32)


def bell_draw(own_key, dims, width, bound, shards=(), kind=jnp.bfloat16):
    drawn = jax.random.normal(own_key, dims, jnp.float32) * width
    if len(shards) > 0:
        drawn = shard_levels(own_key, dims, shards, -0.22, 0.18) * drawn
    return jnp.clip(drawn, min=-bound, max=bound).astype(kind)


def setup_inputs(seed: int = 0) -> dict:
    key_list = jax.random.split(jax.random.key(seed), 10)
    return {
        "sample_ids": place_ends(skewed_ids(key_list[0], (MB, BATCH, TABLES * HOTS), VOCAB, 2), jax.random.fold_in(key_list[0], 3), 0, VOCAB - 1).astype(jnp.int32),
        "id_weights": jnp.clip(0.25 + 1.75 * jax.random.uniform(key_list[1], (MB, BATCH, TABLES * HOTS), jnp.float32) ** shard_levels(key_list[1], (MB, BATCH, TABLES * HOTS), ((1, 32),), -0.2, 0.2), 0.25, 2.0).astype(jnp.bfloat16),
        "dense_features": bell_draw(key_list[2], (MB, BATCH, DIM), 1.0, 6.0, ((1, 32),)),
        "click_labels": place_ends((jax.random.randint(key_list[3], (MB, BATCH), 0, 2) < 1).astype(jnp.int32), jax.random.fold_in(key_list[3], 1), 0, 1),
        "table_shards": bell_draw(key_list[4], (TABLES, VOCAB, DIM), 0.2, 1.1953125, ((0, 16),)),
        "slot_table": jax.random.permutation(key_list[5], TABLES).astype(jnp.int32),
        "top_weight": bell_draw(key_list[6], (TABLES, HIDDEN_SIZE), TABLES ** -0.5, 0.5),
        "top_bias": bell_draw(key_list[7], (HIDDEN_SIZE,), 0.5, 3.0, (), jnp.float32),
        "out_weight": bell_draw(key_list[8], (HIDDEN_SIZE,), HIDDEN_SIZE ** -0.5, 0.1875),
    }


loss_scale = 32768.0

def reference(sample_ids, id_weights, dense_features, click_labels, table_shards, slot_table, top_weight, top_bias, out_weight):
    count = MB * BATCH
    ids_all = sample_ids.reshape(count, TABLES, HOTS)
    weights_all = id_weights.reshape(count, TABLES, HOTS).astype(jnp.float32)
    features = dense_features.reshape(count, DIM).astype(jnp.float32)
    earlier = jnp.arange(HOTS)[None, :] < jnp.arange(HOTS)[:, None]
    scale = 1.0 / jnp.sqrt(jnp.float32(DIM))

    def slot_scores(slot):
        table = slot_table[slot]
        slot_ids = lax.dynamic_index_in_dim(ids_all, table, axis=1, keepdims=False)
        slot_weights = lax.dynamic_index_in_dim(weights_all, table, axis=1, keepdims=False)
        same = slot_ids[:, :, None] == slot_ids[:, None, :]
        summed = lax.optimization_barrier(jnp.sum(jnp.where(same, slot_weights[:, None, :], jnp.float32(0.0)), axis=2))
        first = jnp.logical_not(jnp.any(same & earlier[None], axis=2))
        rounded = lax.optimization_barrier(summed.astype(jnp.bfloat16)).astype(jnp.float32)
        merged = jnp.where(first, rounded, jnp.float32(0.0))
        shard = lax.dynamic_index_in_dim(table_shards, slot, axis=0, keepdims=False)
        rows = shard[slot_ids].astype(jnp.float32)
        pooled = jnp.einsum('nh,nhe->ne', merged, rows).astype(jnp.bfloat16)
        pooled_wide = lax.optimization_barrier(pooled).astype(jnp.float32)
        return (lax.optimization_barrier(jnp.sum(pooled_wide * features, axis=1)) * scale).astype(jnp.bfloat16)
    scores = lax.map(slot_scores, jnp.arange(TABLES, dtype=jnp.int32)).T
    slot_weight = top_weight[slot_table]
    pre = jnp.dot(scores, slot_weight, preferred_element_type=jnp.float32) + top_bias
    gate = jax.nn.sigmoid(pre)
    hidden = (pre * gate).astype(jnp.bfloat16)
    logit_all = jnp.dot(hidden, out_weight, preferred_element_type=jnp.float32)
    labels = click_labels.reshape(count).astype(jnp.float32)
    delta = (jax.nn.sigmoid(logit_all) - labels) * (loss_scale / count)
    slope = gate * (1.0 + pre * (1.0 - gate))
    hidden_grad = (delta[:, None] * out_weight.astype(jnp.float32)[None, :] * slope).astype(jnp.bfloat16)
    hidden_grad = lax.optimization_barrier(hidden_grad)
    grad_slot = jnp.dot(scores.T, hidden_grad, preferred_element_type=jnp.float32)
    grad_bias = lax.optimization_barrier(jnp.sum(hidden_grad.astype(jnp.float32), axis=0))
    grad_top = jnp.zeros_like(grad_slot).at[slot_table].set(grad_slot)
    return (logit_all.reshape(MB, BATCH), grad_top, grad_bias)
```

```python
import functools
import math

import jax
import jax.numpy as jnp
from jax import lax
from jax.experimental import pallas as pl
from jax.experimental.pallas import tpu as pltpu
from jax.sharding import PartitionSpec as P

HOTS = 8
LANES = 128
ROWS = 8
loss_scale = 32768.0
NT = (((1,), (1,)), ((), ()))
MESH = pl.DeviceIdType.MESH
TN = (((0,), (0,)), ((), ()))


def column_of(row):
    size = row.shape[1]
    eye = lax.broadcasted_iota(jnp.int32, (size, size), 0) == lax.broadcasted_iota(jnp.int32, (size, size), 1)
    return jnp.sum(jnp.where(eye, row, 0.0), axis=1, keepdims=True)


def pick_rows(block, spot):
    pick = lax.GatherDimensionNumbers(
        offset_dims=(), collapsed_slice_dims=(0,), start_index_map=(0,),
        operand_batching_dims=(1,), start_indices_batching_dims=(1,))
    return lax.gather(block, spot[..., None], pick, (1, 1), mode=lax.GatherScatterMode.PROMISE_IN_BOUNDS)


def choose_rows(tile_of, spot, bits, first, count):
    if count == 1:
        return pick_rows(tile_of(first), spot)
    half = 1 << ((count - 1).bit_length() - 1)
    low = choose_rows(tile_of, spot, bits, first, half)
    high = choose_rows(tile_of, spot, bits, first + half, count - half)
    return jnp.where(bits[half.bit_length() - 1], high, low)


def row_of(column):
    size = column.shape[0]
    eye = lax.broadcasted_iota(jnp.int32, (size, size), 0) == lax.broadcasted_iota(jnp.int32, (size, size), 1)
    return jnp.sum(jnp.where(eye, column, 0.0), axis=0, keepdims=True)


def step_kernel(count, groups, members, id_ref, weight_ref, table_ref, d_ref, t_ref, place_ref, label_ref, w_ref, b_ref, o_ref,
                logit_ref, top_ref, bias_ref,
                code_ref, turned_ref, x_ref, fin_ref, xs_ref, ds_ref, key_ref, scale_ref, acc_ref, mine_ref,
                got_ref, grad_ref, slope_ref, group_ref, half_ref, part_ref, bias_part,
                x_send, x_recv, d_send, d_recv, s_send, s_recv, g_send, g_recv, p_send, p_recv,
                b_send, b_recv, a_send, a_recv, f_send, f_recv, c_send, c_recv):
    my_g, my_t = lax.axis_index("grp"), lax.axis_index("tab")
    slots, vocab, width = t_ref.shape
    own = x_ref.shape[1] // 2
    samples = x_ref.shape[2]
    hots = own // slots
    blocks = vocab // LANES
    tiles = vocab // ROWS
    tables = got_ref.shape[0]
    hidden = w_ref.shape[1]
    piece = hidden // groups
    per = 2 if members % 2 == 0 else 1
    chunk = per * samples

    def member(k):
        return lax.rem(my_t + k, members)

    def origin(k):
        return lax.rem(my_t - k + members, members)

    def team(k):
        return lax.rem(my_g + k, groups)

    def team_origin(k):
        return lax.rem(my_g - k + groups, groups)

    def remote(src, dst, send, recv, g, t):
        return pltpu.make_async_remote_copy(src_ref=src, dst_ref=dst, send_sem=send, recv_sem=recv,
                                            device_id={"grp": g, "tab": t}, device_id_type=MESH)

    def rows_of(t):
        return pl.ds(pl.multiple_of(t * slots, slots), slots)

    def cols_of(g):
        return pl.ds(pl.multiple_of(g * piece, LANES), piece)

    barrier = pltpu.get_barrier_semaphore()

    @pl.loop(1, members)
    def _(k):
        pl.semaphore_signal(barrier, inc=1, device_id={"grp": my_g, "tab": member(k)}, device_id_type=MESH)

    @pl.loop(1, groups)
    def _(k):
        pl.semaphore_signal(barrier, inc=1, device_id={"grp": team(k), "tab": my_t}, device_id_type=MESH)

    columns = id_ref.shape[2]
    step = LANES // hots
    for c in range(columns // LANES):
        at = slice(c * LANES, (c + 1) * LANES)
        ids = id_ref[:, :, at].reshape(samples, LANES)
        code = jnp.left_shift(LANES + (ids & (LANES - 1)), jnp.right_shift(ids, LANES.bit_length() - 1))
        code = code.astype(jnp.float32).astype(jnp.bfloat16)
        code_ref[c * step : (c + 1) * step] = code.T.astype(jnp.float32).reshape(step, hots, samples)
        share = weight_ref[:, :, at].reshape(samples, LANES)
        turned_ref[c * step : (c + 1) * step] = share.T.astype(jnp.float32).reshape(step, hots, samples)

    @pl.loop(0, members)
    def _(m):
        held = [table_ref[m * slots + s] for s in range(slots)]
        x_ref[m, 0:own] = jnp.concatenate([code_ref[t] for t in held], axis=0).astype(jnp.bfloat16)
        x_ref[m, own : 2 * own] = jnp.concatenate([turned_ref[t] for t in held], axis=0).astype(jnp.bfloat16)

    pl.semaphore_wait(barrier, members + groups - 2)

    def x_copy(k):
        return remote(x_ref.at[member(k)], xs_ref.at[k], x_send.at[k], x_recv.at[k], my_g, member(k))

    def d_copy(k):
        return remote(d_ref, ds_ref.at[k], d_send.at[k], d_recv.at[k], my_g, member(k))

    def s_copy(k):
        return remote(mine_ref.at[k], got_ref.at[rows_of(my_t), :], s_send.at[k], s_recv.at[k], my_g, origin(k))

    @pl.loop(1, members)
    def _(k):
        d_copy(k).start()
        x_copy(k).start()

    xs_ref[0] = x_ref[my_t]
    ds_ref[0] = d_ref[...]

    parts = 2 if vocab % (2 * ROWS) == 0 else 1
    unroll = 4 if slots % 4 == 0 else 1

    @pl.loop(0, members // per)
    def _(i):
        for e in range(per):
            @pl.when(per * i + e > 0)
            def _():
                d_copy(per * i + e).wait_recv()
                x_copy(per * i + e).wait_recv()

        for e in range(per):
            code = xs_ref[per * i + e, 0:own].astype(jnp.float32)
            high = jnp.zeros(code.shape, jnp.int32)
            for k in range(1, blocks):
                high = high + (code >= float(LANES << k)).astype(jnp.int32)
            low = jnp.right_shift(code.astype(jnp.int32), high) & (LANES - 1)
            key_ref[e] = high * LANES + low
            scale_ref[e] = xs_ref[per * i + e, own : 2 * own].astype(jnp.float32)

        def look(slot):
            feats = ds_ref[pl.ds(per * i, per)].reshape(chunk, width)
            size = vocab // parts
            products = [lax.dot_general(t_ref[slot, p * size : (p + 1) * size, :], feats, NT,
                                        preferred_element_type=jnp.float32) for p in range(parts)]
            at = pl.ds(pl.multiple_of(slot * hots, hots), hots)
            for e in range(per):
                key = key_ref[e, at, :]
                high = jnp.right_shift(key, ROWS.bit_length() - 1)
                bits = [(high & (1 << b)) != 0 for b in range((tiles - 1).bit_length())]

                def tile_of(v, e=e):
                    p, r = divmod(v * ROWS, size)
                    return products[p][r : r + ROWS, e * samples : (e + 1) * samples]

                got = choose_rows(tile_of, key & (ROWS - 1), bits, 0, tiles)
                acc_ref[e, at, :] = got * scale_ref[e, at, :]

        @pl.loop(0, slots // unroll)
        def _(q):
            for u in range(unroll):
                look(q * unroll + u)

        for e in range(per):
            total = jnp.sum(acc_ref[e].reshape(slots, hots, samples), axis=1)
            mine_ref[per * i + e] = (total * (1.0 / math.sqrt(width))).astype(jnp.bfloat16).astype(jnp.float32)

        for e in range(per):
            @pl.when(per * i + e > 0)
            def _():
                s_copy(per * i + e).start()

    got_ref[rows_of(my_t), :] = mine_ref[0]

    @pl.loop(1, members)
    def _(k):
        d_copy(k).wait_send()
        x_copy(k).wait_send()
        s_copy(k).wait()

    row = lax.broadcasted_iota(jnp.int32, (tables, tables), 0)
    placed = (place_ref[...] == row).astype(jnp.bfloat16)
    scores = jnp.dot(placed, got_ref[...].astype(jnp.bfloat16), preferred_element_type=jnp.float32)
    scores = scores.astype(jnp.bfloat16)
    pre = lax.dot_general(scores, w_ref[...], TN, preferred_element_type=jnp.float32) + b_ref[...]
    gate = jax.nn.sigmoid(pre)
    value = (pre * gate).astype(jnp.bfloat16).astype(jnp.float32)
    out = o_ref[...].astype(jnp.float32)
    logit = jnp.sum(value * out, axis=1, keepdims=True)
    logit_row = row_of(logit)
    micro, local = logit_ref.shape
    for m in range(micro):
        logit_ref[m : m + 1, :] = logit_row[:, m * local : (m + 1) * local]
    labels = jnp.concatenate([label_ref[m : m + 1, :].astype(jnp.float32) for m in range(micro)], axis=1)
    delta = (jax.nn.sigmoid(logit) - column_of(labels)) * (loss_scale / count)
    slope = gate * (1.0 + pre * (1.0 - gate))
    slope_ref[...] = (delta * out * slope).astype(jnp.bfloat16)
    grad = slope_ref[...]
    grad_ref[pl.ds(tables, 8), :] = jnp.broadcast_to(
        jnp.sum(grad.astype(jnp.float32), axis=0, keepdims=True), (8, hidden))
    grad_ref[pl.ds(0, tables), :] = jnp.dot(scores, grad, preferred_element_type=jnp.float32)

    def g_copy(k):
        return remote(grad_ref.at[:, cols_of(team(k))], group_ref.at[k], g_send.at[k], g_recv.at[k], team(k), my_t)

    @pl.loop(1, groups)
    def _(k):
        g_copy(k).start()

    half_ref[...] = grad_ref[:, cols_of(my_g)]

    @pl.loop(1, groups)
    def _(k):
        g_copy(k).wait()
        half_ref[...] += group_ref[k]

    def p_copy(k):
        return remote(half_ref.at[rows_of(member(k)), :], part_ref.at[k], p_send.at[k], p_recv.at[k], my_g, member(k))

    def b_copy(k):
        return remote(half_ref.at[pl.ds(tables, 1), :], bias_part.at[k], b_send.at[k], b_recv.at[k], my_g, member(k))

    @pl.loop(1, members)
    def _(k):
        p_copy(k).start()

    @pl.loop(1, members)
    def _(k):
        b_copy(k).start()

    part_ref[0] = half_ref[rows_of(my_t), :]
    bias_part[0] = half_ref[tables : tables + 1, :]

    @pl.loop(1, members)
    def _(k):
        p_copy(k).wait()

    fin_ref[my_t, :, cols_of(my_g)] = jnp.sum(part_ref[...], axis=0).astype(jnp.bfloat16)

    def a_copy(k):
        at = fin_ref.at[my_t, :, cols_of(my_g)]
        return remote(at, at, a_send.at[k], a_recv.at[k], my_g, member(k))

    def f_copy(k, j):
        at = fin_ref.at[origin(k), :, cols_of(my_g)]
        return remote(at, at, f_send.at[j, k], f_recv.at[j, k], team(j), my_t)

    def c_copy(j):
        at = bias_ref.at[:, cols_of(my_g)]
        return remote(at, at, c_send.at[j], c_recv.at[j], team(j), my_t)

    @pl.loop(1, members)
    def _(k):
        a_copy(k).start()

    @pl.loop(1, groups)
    def _(j):
        f_copy(0, j).start()

    @pl.loop(1, members)
    def _(k):
        b_copy(k).wait()

    def add(q, total):
        return total + bias_part[lax.rem(my_t - q + members, members)]

    bias_ref[:, cols_of(my_g)] = lax.fori_loop(1, members, add, bias_part[my_t])

    @pl.loop(1, groups)
    def _(j):
        c_copy(j).start()

    @pl.loop(1, members)
    def _(k):
        a_copy(k).wait_recv()

        @pl.loop(1, groups)
        def _(j):
            f_copy(k, j).start()

    @pl.loop(1, members)
    def _(k):
        a_copy(k).wait_send()

    @pl.loop(1, groups)
    def _(j):
        c_copy(j).wait()

        @pl.loop(0, members)
        def _(k):
            f_copy(k, j).wait()

    for m in range(members):
        top_ref[m * slots : (m + 1) * slots, :] = fin_ref[m].astype(jnp.float32)


def fused_step(count, groups, members, ids, id_weights, d, table, slot_table, labels, weight, bias, out):
    samples, width = d.shape
    slots, vocab, _ = table.shape
    tables, hidden = weight.shape
    piece = hidden // groups
    per = 2 if members % 2 == 0 else 1
    hots = ids.shape[2] // tables
    own = slots * hots
    vmem = pl.BlockSpec(memory_space=pltpu.VMEM)
    smem = pl.BlockSpec(memory_space=pltpu.SMEM)
    f32, bf16 = jnp.float32, jnp.bfloat16
    dma = pltpu.SemaphoreType.DMA
    return pl.pallas_call(
        functools.partial(step_kernel, count, groups, members),
        out_shape=(
            jax.ShapeDtypeStruct(labels.shape, f32),
            jax.ShapeDtypeStruct((tables, hidden), f32),
            jax.ShapeDtypeStruct((1, hidden), f32),
        ),
        in_specs=[vmem] * 2 + [smem] + [vmem] * 7,
        out_specs=(vmem,) * 3,
        scratch_shapes=[
            pltpu.VMEM((tables, hots, samples), f32),
            pltpu.VMEM((tables, hots, samples), f32),
            pltpu.VMEM((members, 2 * own, samples), bf16),
            pltpu.VMEM((members, slots, hidden), bf16),
            pltpu.VMEM((members, 2 * own, samples), bf16),
            pltpu.VMEM((members, samples, width), bf16),
            pltpu.VMEM((per, own, samples), jnp.int32),
            pltpu.VMEM((per, own, samples), f32),
            pltpu.VMEM((per, own, samples), f32),
            pltpu.VMEM((members, slots, samples), f32),
            pltpu.VMEM((tables, samples), f32),
            pltpu.VMEM((tables + 8, hidden), f32),
            pltpu.VMEM((samples, hidden), bf16),
            pltpu.VMEM((groups, tables + 8, piece), f32),
            pltpu.VMEM((tables + 8, piece), f32),
            pltpu.VMEM((members, slots, piece), f32),
            pltpu.VMEM((members, 1, piece), f32),
        ]
        + [dma((members,))] * 6 + [dma((groups,))] * 2 + [dma((members,))] * 6
        + [dma((groups, members))] * 2 + [dma((groups,))] * 2,
        compiler_params=pltpu.CompilerParams(collective_id=1, has_side_effects=True),
    )(ids, id_weights, slot_table, d, table, slot_table.reshape(1, -1), labels, weight, bias.reshape(1, -1), out.reshape(1, -1))


def per_device(
    sample_ids, id_weights, dense_features, click_labels, table_shards, slot_table, top_weight, top_bias, out_weight
):
    micro, local_batch, columns = sample_ids.shape
    tables = slot_table.shape[0]
    slots = table_shards.shape[0]
    width = dense_features.shape[2]
    hidden = top_weight.shape[1]
    members = lax.axis_size("tab")
    groups = lax.axis_size("grp")
    samples = micro * local_batch
    count = samples * groups * members
    logit, grad_top, grad_bias = fused_step(
        count, groups, members, sample_ids, id_weights, dense_features.reshape(samples, width), table_shards,
        slot_table, click_labels, top_weight, top_bias, out_weight
    )
    return (logit, grad_top, grad_bias.reshape(hidden))


def solution(mesh):
    return jax.shard_map(
        per_device,
        mesh=mesh,
        in_specs=(
            P(None, ("grp", "tab"), None),
            P(None, ("grp", "tab"), None),
            P(None, ("grp", "tab"), None),
            P(None, ("grp", "tab")),
            P("tab", None, None),
            P(),
            P(),
            P(),
            P(),
        ),
        out_specs=(P(None, ("grp", "tab")), P(), P()),
        check_vma=False,
    )
```

```python
import functools
import math

import jax
import jax.numpy as jnp
from jax import lax
from jax.experimental import pallas as pl
from jax.experimental.pallas import tpu as pltpu
from jax.sharding import PartitionSpec as P

HOTS = 8
LANES = 128
ROWS = 8
loss_scale = 32768.0
NT = (((1,), (1,)), ((), ()))
MESH = pl.DeviceIdType.MESH
TN = (((0,), (0,)), ((), ()))


def column_of(row):
    size = row.shape[1]
    eye = lax.broadcasted_iota(jnp.int32, (size, size), 0) == lax.broadcasted_iota(jnp.int32, (size, size), 1)
    return jnp.sum(jnp.where(eye, row, 0.0), axis=1, keepdims=True)


def pick_rows(block, spot):
    pick = lax.GatherDimensionNumbers(
        offset_dims=(), collapsed_slice_dims=(0,), start_index_map=(0,),
        operand_batching_dims=(1,), start_indices_batching_dims=(1,))
    return lax.gather(block, spot[..., None], pick, (1, 1), mode=lax.GatherScatterMode.PROMISE_IN_BOUNDS)


def choose_rows(tile_of, spot, bits, first, count):
    if count == 1:
        return pick_rows(tile_of(first), spot)
    half = 1 << ((count - 1).bit_length() - 1)
    low = choose_rows(tile_of, spot, bits, first, half)
    high = choose_rows(tile_of, spot, bits, first + half, count - half)
    return jnp.where(bits[half.bit_length() - 1], high, low)


def row_of(column):
    size = column.shape[0]
    eye = lax.broadcasted_iota(jnp.int32, (size, size), 0) == lax.broadcasted_iota(jnp.int32, (size, size), 1)
    return jnp.sum(jnp.where(eye, column, 0.0), axis=0, keepdims=True)


def step_kernel(count, groups, members, id_ref, weight_ref, table_ref, d_ref, t_ref, place_ref, label_ref, w_ref, b_ref, o_ref,
                logit_ref, top_ref, bias_ref,
                code_ref, turned_ref, x_ref, fin_ref, xs_ref, ds_ref, key_ref, scale_ref, acc_ref, mine_ref,
                got_ref, grad_ref, slope_ref, group_ref, half_ref, part_ref, bias_part,
                x_send, x_recv, d_send, d_recv, s_send, s_recv, g_send, g_recv, p_send, p_recv,
                b_send, b_recv, a_send, a_recv, f_send, f_recv, c_send, c_recv):
    my_g, my_t = lax.axis_index("grp"), lax.axis_index("tab")
    slots, vocab, width = t_ref.shape
    own = x_ref.shape[1] // 2
    samples = x_ref.shape[2]
    hots = own // slots
    blocks = vocab // LANES
    tiles = vocab // ROWS
    tables = got_ref.shape[0]
    hidden = w_ref.shape[1]
    piece = hidden // groups
    per = 2 if members % 2 == 0 else 1
    chunk = per * samples

    plane = max(n for n in range(1, members + 1) if members % n == 0 and n * n <= members)
    lines = members // plane
    even = members & (members - 1) == 0

    def move(k, way):
        if even:
            spot = 0
            for bit in range(members.bit_length() - 1):
                spot = spot + lax.rem(lax.div(my_t, 1 << bit) + lax.div(k, 1 << bit), 2) * (1 << bit)
            return spot
        line = lax.rem(lax.div(my_t, plane) + way * lax.div(k, plane) + lines, lines)
        return line * plane + lax.rem(lax.rem(my_t, plane) + way * lax.rem(k, plane) + plane, plane)

    def member(k):
        return move(jnp.int32(k), 1)

    def origin(k):
        return move(jnp.int32(k), -1)

    def team(k):
        return lax.rem(my_g + k, groups)

    def team_origin(k):
        return lax.rem(my_g - k + groups, groups)

    def remote(src, dst, send, recv, g, t):
        return pltpu.make_async_remote_copy(src_ref=src, dst_ref=dst, send_sem=send, recv_sem=recv,
                                            device_id={"grp": g, "tab": t}, device_id_type=MESH)

    def rows_of(t):
        return pl.ds(pl.multiple_of(t * slots, slots), slots)

    def cols_of(g):
        return pl.ds(pl.multiple_of(g * piece, LANES), piece)

    barrier = pltpu.get_barrier_semaphore()

    @pl.loop(1, members)
    def _(k):
        pl.semaphore_signal(barrier, inc=1, device_id={"grp": my_g, "tab": member(k)}, device_id_type=MESH)

    @pl.loop(1, groups)
    def _(k):
        pl.semaphore_signal(barrier, inc=1, device_id={"grp": team(k), "tab": my_t}, device_id_type=MESH)

    columns = id_ref.shape[2]
    step = LANES // hots
    for c in range(columns // LANES):
        at = slice(c * LANES, (c + 1) * LANES)
        ids = id_ref[:, :, at].reshape(samples, LANES)
        code = jnp.left_shift(LANES + (ids & (LANES - 1)), jnp.right_shift(ids, LANES.bit_length() - 1))
        code = code.astype(jnp.float32).astype(jnp.bfloat16)
        code_ref[c * step : (c + 1) * step] = code.T.astype(jnp.float32).reshape(step, hots, samples)
        share = weight_ref[:, :, at].reshape(samples, LANES)
        turned_ref[c * step : (c + 1) * step] = share.T.astype(jnp.float32).reshape(step, hots, samples)

    @pl.loop(0, members)
    def _(m):
        held = [table_ref[m * slots + s] for s in range(slots)]
        x_ref[m, 0:own] = jnp.concatenate([code_ref[t] for t in held], axis=0).astype(jnp.bfloat16)
        x_ref[m, own : 2 * own] = jnp.concatenate([turned_ref[t] for t in held], axis=0).astype(jnp.bfloat16)

    pl.semaphore_wait(barrier, members + groups - 2)

    def x_copy(k):
        return remote(x_ref.at[member(k)], xs_ref.at[k], x_send.at[k], x_recv.at[k], my_g, member(k))

    def d_copy(k):
        return remote(d_ref, ds_ref.at[k], d_send.at[k], d_recv.at[k], my_g, member(k))

    def pass_copy(line, k):
        at = line * plane + k
        return remote(ds_ref.at[line * plane], ds_ref.at[at], d_send.at[at], d_recv.at[at], my_g, member(k))

    def s_copy(k):
        return remote(mine_ref.at[k], got_ref.at[rows_of(my_t), :], s_send.at[k], s_recv.at[k], my_g, origin(k))

    @pl.loop(1, lines)
    def _(line):
        d_copy(line * plane).start()

    @pl.loop(1, plane)
    def _(k):
        d_copy(k).start()

    for k in range(1, per):
        x_copy(k).start()

    @pl.loop(2 * per, members)
    def _(k):
        x_copy(k).start()

    @pl.loop(per, min(2 * per, members))
    def _(k):
        x_copy(k).start()

    xs_ref[0] = x_ref[my_t]
    ds_ref[0] = d_ref[...]

    parts = 2 if vocab % (2 * ROWS) == 0 else 1
    unroll = 4 if slots % 4 == 0 else 1

    turns = members // per

    @pl.loop(0, turns)
    def _(turn):
        @pl.when(turn == 1)
        def _():
            @pl.loop(1, lines)
            def _(line):
                d_copy(line * plane).wait_recv()

                @pl.loop(1, plane)
                def _(k):
                    pass_copy(line, k).start()

        i = lax.div(turn + turns - 2, turns - 1) * (1 + lax.rem(turn, turns - 1)) if turns > 1 else turn

        for e in range(per):
            @pl.when(lax.rem(per * i + e, plane) > 0)
            def _():
                d_copy(per * i + e).wait_recv()

            @pl.when(per * i + e > 0)
            def _():
                x_copy(per * i + e).wait_recv()

        for e in range(per):
            code = xs_ref[per * i + e, 0:own].astype(jnp.float32)
            high = jnp.zeros(code.shape, jnp.int32)
            for k in range(1, blocks):
                high = high + (code >= float(LANES << k)).astype(jnp.int32)
            low = jnp.right_shift(code.astype(jnp.int32), high) & (LANES - 1)
            key_ref[e] = high * LANES + low
            scale_ref[e] = xs_ref[per * i + e, own : 2 * own].astype(jnp.float32)

        def look(slot):
            feats = ds_ref[pl.ds(per * i, per)].reshape(chunk, width)
            size = vocab // parts
            products = [lax.dot_general(t_ref[slot, p * size : (p + 1) * size, :], feats, NT,
                                        preferred_element_type=jnp.float32) for p in range(parts)]
            at = pl.ds(pl.multiple_of(slot * hots, hots), hots)
            for e in range(per):
                key = key_ref[e, at, :]
                high = jnp.right_shift(key, ROWS.bit_length() - 1)
                bits = [(high & (1 << b)) != 0 for b in range((tiles - 1).bit_length())]

                def tile_of(v, e=e):
                    p, r = divmod(v * ROWS, size)
                    return products[p][r : r + ROWS, e * samples : (e + 1) * samples]

                got = choose_rows(tile_of, key & (ROWS - 1), bits, 0, tiles)
                acc_ref[e, at, :] = got * scale_ref[e, at, :]

        @pl.loop(0, slots // unroll)
        def _(q):
            for u in range(unroll):
                look(q * unroll + u)

        for e in range(per):
            total = jnp.sum(acc_ref[e].reshape(slots, hots, samples), axis=1)
            mine_ref[per * i + e] = (total * (1.0 / math.sqrt(width))).astype(jnp.bfloat16).astype(jnp.float32)

        for e in range(per):
            @pl.when(per * i + e > 0)
            def _():
                s_copy(per * i + e).start()

    got_ref[rows_of(my_t), :] = mine_ref[0]

    @pl.loop(1, members)
    def _(k):
        d_copy(k).wait_send()
        x_copy(k).wait_send()
        s_copy(k).wait()

    row = lax.broadcasted_iota(jnp.int32, (tables, tables), 0)
    placed = (place_ref[...] == row).astype(jnp.bfloat16)
    scores = jnp.dot(placed, got_ref[...].astype(jnp.bfloat16), preferred_element_type=jnp.float32)
    scores = scores.astype(jnp.bfloat16)
    pre = lax.dot_general(scores, w_ref[...], TN, preferred_element_type=jnp.float32) + b_ref[...]
    gate = jax.nn.sigmoid(pre)
    value = (pre * gate).astype(jnp.bfloat16).astype(jnp.float32)
    out = o_ref[...].astype(jnp.float32)
    logit = jnp.sum(value * out, axis=1, keepdims=True)
    logit_row = row_of(logit)
    micro, local = logit_ref.shape
    for m in range(micro):
        logit_ref[m : m + 1, :] = logit_row[:, m * local : (m + 1) * local]
    labels = jnp.concatenate([label_ref[m : m + 1, :].astype(jnp.float32) for m in range(micro)], axis=1)
    delta = (jax.nn.sigmoid(logit) - column_of(labels)) * (loss_scale / count)
    slope = gate * (1.0 + pre * (1.0 - gate))
    slope_ref[...] = (delta * out * slope).astype(jnp.bfloat16)
    grad = slope_ref[...]
    grad_ref[pl.ds(tables, 8), :] = jnp.broadcast_to(
        jnp.sum(grad.astype(jnp.float32), axis=0, keepdims=True), (8, hidden))
    grad_ref[pl.ds(0, tables), :] = jnp.dot(scores, grad, preferred_element_type=jnp.float32)

    def g_copy(k):
        return remote(grad_ref.at[:, cols_of(team(k))], group_ref.at[k], g_send.at[k], g_recv.at[k], team(k), my_t)

    @pl.loop(1, groups)
    def _(k):
        g_copy(k).start()

    half_ref[...] = grad_ref[:, cols_of(my_g)]

    @pl.loop(1, groups)
    def _(k):
        g_copy(k).wait()
        half_ref[...] += group_ref[k]

    def p_copy(k):
        return remote(half_ref.at[rows_of(member(k)), :], part_ref.at[k], p_send.at[k], p_recv.at[k], my_g, member(k))

    def b_copy(k):
        return remote(half_ref.at[pl.ds(tables, 1), :], bias_part.at[k], b_send.at[k], b_recv.at[k], my_g, member(k))

    @pl.loop(1, members)
    def _(k):
        p_copy(k).start()

    @pl.loop(1, members)
    def _(k):
        b_copy(k).start()

    part_ref[0] = half_ref[rows_of(my_t), :]
    bias_part[0] = half_ref[tables : tables + 1, :]

    @pl.loop(1, members)
    def _(k):
        p_copy(k).wait()

    fin_ref[my_t, :, cols_of(my_g)] = jnp.sum(part_ref[...], axis=0).astype(jnp.bfloat16)

    def a_copy(k):
        at = fin_ref.at[my_t, :, cols_of(my_g)]
        return remote(at, at, a_send.at[k], a_recv.at[k], my_g, member(k))

    def f_copy(k, j):
        at = fin_ref.at[origin(k), :, cols_of(my_g)]
        return remote(at, at, f_send.at[j, k], f_recv.at[j, k], team(j), my_t)

    def c_copy(j):
        at = bias_ref.at[:, cols_of(my_g)]
        return remote(at, at, c_send.at[j], c_recv.at[j], team(j), my_t)

    @pl.loop(1, members)
    def _(k):
        a_copy(k).start()

    @pl.loop(1, groups)
    def _(j):
        f_copy(0, j).start()

    @pl.loop(1, members)
    def _(k):
        b_copy(k).wait()

    def add(q, total):
        return total + bias_part[lax.rem(my_t - q + members, members)]

    bias_ref[:, cols_of(my_g)] = lax.fori_loop(1, members, add, bias_part[my_t])

    @pl.loop(1, groups)
    def _(j):
        c_copy(j).start()

    @pl.loop(1, members)
    def _(k):
        a_copy(k).wait_recv()

        @pl.loop(1, groups)
        def _(j):
            f_copy(k, j).start()

    @pl.loop(1, members)
    def _(k):
        a_copy(k).wait_send()

    @pl.loop(1, groups)
    def _(j):
        c_copy(j).wait()

        @pl.loop(0, members)
        def _(k):
            f_copy(k, j).wait()

    for m in range(members):
        top_ref[m * slots : (m + 1) * slots, :] = fin_ref[m].astype(jnp.float32)


def fused_step(count, groups, members, ids, id_weights, d, table, slot_table, labels, weight, bias, out):
    samples, width = d.shape
    slots, vocab, _ = table.shape
    tables, hidden = weight.shape
    piece = hidden // groups
    per = 2 if members % 2 == 0 else 1
    hots = ids.shape[2] // tables
    own = slots * hots
    vmem = pl.BlockSpec(memory_space=pltpu.VMEM)
    smem = pl.BlockSpec(memory_space=pltpu.SMEM)
    f32, bf16 = jnp.float32, jnp.bfloat16
    dma = pltpu.SemaphoreType.DMA
    return pl.pallas_call(
        functools.partial(step_kernel, count, groups, members),
        out_shape=(
            jax.ShapeDtypeStruct(labels.shape, f32),
            jax.ShapeDtypeStruct((tables, hidden), f32),
            jax.ShapeDtypeStruct((1, hidden), f32),
        ),
        in_specs=[vmem] * 2 + [smem] + [vmem] * 7,
        out_specs=(vmem,) * 3,
        scratch_shapes=[
            pltpu.VMEM((tables, hots, samples), f32),
            pltpu.VMEM((tables, hots, samples), f32),
            pltpu.VMEM((members, 2 * own, samples), bf16),
            pltpu.VMEM((members, slots, hidden), bf16),
            pltpu.VMEM((members, 2 * own, samples), bf16),
            pltpu.VMEM((members, samples, width), bf16),
            pltpu.VMEM((per, own, samples), jnp.int32),
            pltpu.VMEM((per, own, samples), f32),
            pltpu.VMEM((per, own, samples), f32),
            pltpu.VMEM((members, slots, samples), f32),
            pltpu.VMEM((tables, samples), f32),
            pltpu.VMEM((tables + 8, hidden), f32),
            pltpu.VMEM((samples, hidden), bf16),
            pltpu.VMEM((groups, tables + 8, piece), f32),
            pltpu.VMEM((tables + 8, piece), f32),
            pltpu.VMEM((members, slots, piece), f32),
            pltpu.VMEM((members, 1, piece), f32),
        ]
        + [dma((members,))] * 6 + [dma((groups,))] * 2 + [dma((members,))] * 6
        + [dma((groups, members))] * 2 + [dma((groups,))] * 2,
        compiler_params=pltpu.CompilerParams(collective_id=1, has_side_effects=True),
    )(ids, id_weights, slot_table, d, table, slot_table.reshape(1, -1), labels, weight, bias.reshape(1, -1), out.reshape(1, -1))


def per_device(
    sample_ids, id_weights, dense_features, click_labels, table_shards, slot_table, top_weight, top_bias, out_weight
):
    micro, local_batch, columns = sample_ids.shape
    tables = slot_table.shape[0]
    slots = table_shards.shape[0]
    width = dense_features.shape[2]
    hidden = top_weight.shape[1]
    members = lax.axis_size("tab")
    groups = lax.axis_size("grp")
    samples = micro * local_batch
    count = samples * groups * members
    logit, grad_top, grad_bias = fused_step(
        count, groups, members, sample_ids, id_weights, dense_features.reshape(samples, width), table_shards,
        slot_table, click_labels, top_weight, top_bias, out_weight
    )
    return (logit, grad_top, grad_bias.reshape(hidden))


def solution(mesh):
    return jax.shard_map(
        per_device,
        mesh=mesh,
        in_specs=(
            P(None, ("grp", "tab"), None),
            P(None, ("grp", "tab"), None),
            P(None, ("grp", "tab"), None),
            P(None, ("grp", "tab")),
            P("tab", None, None),
            P(),
            P(),
            P(),
            P(),
        ),
        out_specs=(P(None, ("grp", "tab")), P(), P()),
        check_vma=False,
    )
```

```python
import functools
import math

import jax
import jax.numpy as jnp
from jax import lax
from jax.experimental import pallas as pl
from jax.experimental.pallas import tpu as pltpu
from jax.sharding import PartitionSpec as P

HOTS = 8
LANES = 128
ROWS = 8
loss_scale = 32768.0
NT = (((1,), (1,)), ((), ()))
MESH = pl.DeviceIdType.MESH
TN = (((0,), (0,)), ((), ()))


def column_of(row):
    size = row.shape[1]
    eye = lax.broadcasted_iota(jnp.int32, (size, size), 0) == lax.broadcasted_iota(jnp.int32, (size, size), 1)
    return jnp.sum(jnp.where(eye, row, 0.0), axis=1, keepdims=True)


def pick_rows(block, spot):
    pick = lax.GatherDimensionNumbers(
        offset_dims=(), collapsed_slice_dims=(0,), start_index_map=(0,),
        operand_batching_dims=(1,), start_indices_batching_dims=(1,))
    return lax.gather(block, spot[..., None], pick, (1, 1), mode=lax.GatherScatterMode.PROMISE_IN_BOUNDS)


def choose_rows(tile_of, spot, bits, first, count):
    if count == 1:
        return pick_rows(tile_of(first), spot)
    half = 1 << ((count - 1).bit_length() - 1)
    low = choose_rows(tile_of, spot, bits, first, half)
    high = choose_rows(tile_of, spot, bits, first + half, count - half)
    return jnp.where(bits[half.bit_length() - 1], high, low)


def row_of(column):
    size = column.shape[0]
    eye = lax.broadcasted_iota(jnp.int32, (size, size), 0) == lax.broadcasted_iota(jnp.int32, (size, size), 1)
    return jnp.sum(jnp.where(eye, column, 0.0), axis=0, keepdims=True)


def step_kernel(count, groups, members, ids, weights, table_of, feats_in, shards, place_in, labels_in, top_in, bias_in, out_in,
                logit_out, top_out, bias_out,
                id_ref, weight_ref, table_ref, t_ref, place_ref, label_ref, w_ref, b_ref, o_ref, logit_ref, bias_ref,
                load_sem, store_sem, code_ref, turned_ref, x_ref, fin_ref, xs_ref, ds_ref, key_ref, scale_ref, acc_ref, mine_ref,
                got_ref, grad_ref, slope_ref, group_ref, half_ref, part_ref, bias_part,
                x_send, x_recv, d_send, d_recv, s_send, s_recv, g_send, g_recv, p_send, p_recv,
                b_send, b_recv, a_send, a_recv, f_send, f_recv, c_send, c_recv):
    my_g, my_t = lax.axis_index("grp"), lax.axis_index("tab")
    slots, vocab, width = t_ref.shape
    micro, local, columns = id_ref.shape
    own = x_ref.shape[1] // 2
    samples = x_ref.shape[2]
    hots = own // slots
    blocks = vocab // LANES
    tiles = vocab // ROWS
    tables = got_ref.shape[0]
    hidden = w_ref.shape[1]
    piece = hidden // groups
    per = 2 if members % 2 == 0 else 1
    chunk = per * samples

    plane = max(n for n in range(1, members + 1) if members % n == 0 and n * n <= members)
    lines = members // plane
    even = members & (members - 1) == 0

    def move(k, way):
        if even:
            spot = 0
            for bit in range(members.bit_length() - 1):
                spot = spot + lax.rem(lax.div(my_t, 1 << bit) + lax.div(k, 1 << bit), 2) * (1 << bit)
            return spot
        line = lax.rem(lax.div(my_t, plane) + way * lax.div(k, plane) + lines, lines)
        return line * plane + lax.rem(lax.rem(my_t, plane) + way * lax.rem(k, plane) + plane, plane)

    def member(k):
        return move(jnp.int32(k), 1)

    def origin(k):
        return move(jnp.int32(k), -1)

    def team(k):
        return lax.rem(my_g + k, groups)

    def team_origin(k):
        return lax.rem(my_g - k + groups, groups)

    def remote(src, dst, send, recv, g, t):
        return pltpu.make_async_remote_copy(src_ref=src, dst_ref=dst, send_sem=send, recv_sem=recv,
                                            device_id={"grp": g, "tab": t}, device_id_type=MESH)

    def rows_of(t):
        return pl.ds(pl.multiple_of(t * slots, slots), slots)

    def cols_of(g):
        return pl.ds(pl.multiple_of(g * piece, LANES), piece)

    barrier = pltpu.get_barrier_semaphore()

    @pl.loop(1, members)
    def _(k):
        pl.semaphore_signal(barrier, inc=1, device_id={"grp": my_g, "tab": member(k)}, device_id_type=MESH)

    @pl.loop(1, groups)
    def _(k):
        pl.semaphore_signal(barrier, inc=1, device_id={"grp": team(k), "tab": my_t}, device_id_type=MESH)

    loads = [pltpu.make_async_copy(src, dst, load_sem.at[n]) for n, (src, dst) in enumerate((
        (table_of, table_ref), (ids, id_ref), (weights, weight_ref), (feats_in, ds_ref.at[0]), (shards, t_ref),
        (place_in, place_ref), (labels_in, label_ref), (top_in, w_ref), (bias_in, b_ref), (out_in, o_ref)))]
    for load in loads:
        load.start()
    for load in loads[:3]:
        load.wait()

    step = LANES // hots
    for c in range(columns // LANES):
        at = slice(c * LANES, (c + 1) * LANES)
        ids = id_ref[:, :, at].reshape(samples, LANES)
        code = jnp.left_shift(LANES + (ids & (LANES - 1)), jnp.right_shift(ids, LANES.bit_length() - 1))
        code = code.astype(jnp.float32).astype(jnp.bfloat16)
        code_ref[c * step : (c + 1) * step] = code.T.astype(jnp.float32).reshape(step, hots, samples)
        share = weight_ref[:, :, at].reshape(samples, LANES)
        turned_ref[c * step : (c + 1) * step] = share.T.astype(jnp.float32).reshape(step, hots, samples)

    @pl.loop(0, members)
    def _(m):
        held = [table_ref[m * slots + s] for s in range(slots)]
        x_ref[m, 0:own] = jnp.concatenate([code_ref[t] for t in held], axis=0).astype(jnp.bfloat16)
        x_ref[m, own : 2 * own] = jnp.concatenate([turned_ref[t] for t in held], axis=0).astype(jnp.bfloat16)

    loads[3].wait()
    pl.semaphore_wait(barrier, members + groups - 2)

    def x_copy(k):
        return remote(x_ref.at[member(k)], xs_ref.at[k], x_send.at[k], x_recv.at[k], my_g, member(k))

    def d_copy(k):
        return remote(ds_ref.at[0], ds_ref.at[k], d_send.at[k], d_recv.at[k], my_g, member(k))

    def pass_copy(line, k):
        at = line * plane + k
        return remote(ds_ref.at[line * plane], ds_ref.at[at], d_send.at[at], d_recv.at[at], my_g, member(k))

    def s_copy(k):
        return remote(mine_ref.at[k], got_ref.at[rows_of(my_t), :], s_send.at[k], s_recv.at[k], my_g, origin(k))

    @pl.loop(1, lines)
    def _(line):
        d_copy(line * plane).start()

    @pl.loop(1, plane)
    def _(k):
        d_copy(k).start()

    for k in range(1, per):
        x_copy(k).start()

    @pl.loop(2 * per, members)
    def _(k):
        x_copy(k).start()

    @pl.loop(per, min(2 * per, members))
    def _(k):
        x_copy(k).start()

    xs_ref[0] = x_ref[my_t]
    loads[4].wait()

    parts = 2 if vocab % (2 * ROWS) == 0 else 1
    unroll = 4 if slots % 4 == 0 else 1

    turns = members // per

    @pl.loop(0, turns)
    def _(turn):
        @pl.when(turn == 1)
        def _():
            @pl.loop(1, lines)
            def _(line):
                d_copy(line * plane).wait_recv()

                @pl.loop(1, plane)
                def _(k):
                    pass_copy(line, k).start()

        i = lax.div(turn + turns - 2, turns - 1) * (1 + lax.rem(turn, turns - 1)) if turns > 1 else turn

        for e in range(per):
            @pl.when(lax.rem(per * i + e, plane) > 0)
            def _():
                d_copy(per * i + e).wait_recv()

            @pl.when(per * i + e > 0)
            def _():
                x_copy(per * i + e).wait_recv()

        for e in range(per):
            code = xs_ref[per * i + e, 0:own].astype(jnp.float32)
            high = jnp.zeros(code.shape, jnp.int32)
            for k in range(1, blocks):
                high = high + (code >= float(LANES << k)).astype(jnp.int32)
            low = jnp.right_shift(code.astype(jnp.int32), high) & (LANES - 1)
            key_ref[e] = high * LANES + low
            scale_ref[e] = xs_ref[per * i + e, own : 2 * own].astype(jnp.float32)

        def look(slot):
            feats = ds_ref[pl.ds(per * i, per)].reshape(chunk, width)
            size = vocab // parts
            products = [lax.dot_general(t_ref[slot, p * size : (p + 1) * size, :], feats, NT,
                                        preferred_element_type=jnp.float32) for p in range(parts)]
            at = pl.ds(pl.multiple_of(slot * hots, hots), hots)
            for e in range(per):
                key = key_ref[e, at, :]
                high = jnp.right_shift(key, ROWS.bit_length() - 1)
                bits = [(high & (1 << b)) != 0 for b in range((tiles - 1).bit_length())]

                def tile_of(v, e=e):
                    p, r = divmod(v * ROWS, size)
                    return products[p][r : r + ROWS, e * samples : (e + 1) * samples]

                got = choose_rows(tile_of, key & (ROWS - 1), bits, 0, tiles)
                acc_ref[e, at, :] = got * scale_ref[e, at, :]

        @pl.loop(0, slots // unroll)
        def _(q):
            for u in range(unroll):
                look(q * unroll + u)

        for e in range(per):
            total = jnp.sum(acc_ref[e].reshape(slots, hots, samples), axis=1)
            mine_ref[per * i + e] = (total * (1.0 / math.sqrt(width))).astype(jnp.bfloat16).astype(jnp.float32)

        for e in range(per):
            @pl.when(per * i + e > 0)
            def _():
                s_copy(per * i + e).start()

    got_ref[rows_of(my_t), :] = mine_ref[0]

    @pl.loop(1, members)
    def _(k):
        d_copy(k).wait_send()
        x_copy(k).wait_send()
        s_copy(k).wait()

    for load in loads[5:]:
        load.wait()
    row = lax.broadcasted_iota(jnp.int32, (tables, tables), 0)
    placed = (place_ref[...] == row).astype(jnp.bfloat16)
    scores = jnp.dot(placed, got_ref[...].astype(jnp.bfloat16), preferred_element_type=jnp.float32)
    scores = scores.astype(jnp.bfloat16)
    pre = lax.dot_general(scores, w_ref[...], TN, preferred_element_type=jnp.float32) + b_ref[...]
    gate = jax.nn.sigmoid(pre)
    value = (pre * gate).astype(jnp.bfloat16).astype(jnp.float32)
    out = o_ref[...].astype(jnp.float32)
    out = jnp.concatenate([out[r : r + 1, :] for r in range(out.shape[0])], axis=1)
    logit = jnp.sum(value * out, axis=1, keepdims=True)
    logit_row = row_of(logit)
    for m in range(micro):
        logit_ref[m : m + 1, :] = logit_row[:, m * local : (m + 1) * local]
    logit_store = pltpu.make_async_copy(logit_ref, logit_out, store_sem.at[0])
    logit_store.start()
    labels = jnp.concatenate([label_ref[m : m + 1, :].astype(jnp.float32) for m in range(micro)], axis=1)
    delta = (jax.nn.sigmoid(logit) - column_of(labels)) * (loss_scale / count)
    slope = gate * (1.0 + pre * (1.0 - gate))
    slope_ref[...] = (delta * out * slope).astype(jnp.bfloat16)
    grad = slope_ref[...]
    grad_ref[pl.ds(tables, 8), :] = jnp.broadcast_to(
        jnp.sum(grad.astype(jnp.float32), axis=0, keepdims=True), (8, hidden))
    grad_ref[pl.ds(0, tables), :] = jnp.dot(scores, grad, preferred_element_type=jnp.float32)

    def g_copy(k):
        return remote(grad_ref.at[:, cols_of(team(k))], group_ref.at[k], g_send.at[k], g_recv.at[k], team(k), my_t)

    @pl.loop(1, groups)
    def _(k):
        g_copy(k).start()

    half_ref[...] = grad_ref[:, cols_of(my_g)]

    @pl.loop(1, groups)
    def _(k):
        g_copy(k).wait()
        half_ref[...] += group_ref[k]

    def p_copy(k):
        return remote(half_ref.at[rows_of(member(k)), :], part_ref.at[k], p_send.at[k], p_recv.at[k], my_g, member(k))

    def b_copy(k):
        return remote(half_ref.at[pl.ds(tables, 1), :], bias_part.at[k], b_send.at[k], b_recv.at[k], my_g, member(k))

    @pl.loop(1, members)
    def _(k):
        p_copy(k).start()

    @pl.loop(1, members)
    def _(k):
        b_copy(k).start()

    part_ref[0] = half_ref[rows_of(my_t), :]
    bias_part[0] = half_ref[tables : tables + 1, :]

    @pl.loop(1, members)
    def _(k):
        p_copy(k).wait()

    fin_ref[my_t, :, cols_of(my_g)] = jnp.sum(part_ref[...], axis=0).astype(jnp.bfloat16)

    def a_copy(k):
        at = fin_ref.at[my_t, :, cols_of(my_g)]
        return remote(at, at, a_send.at[k], a_recv.at[k], my_g, member(k))

    def f_copy(k, j):
        at = fin_ref.at[origin(k), :, cols_of(my_g)]
        return remote(at, at, f_send.at[j, k], f_recv.at[j, k], team(j), my_t)

    def c_copy(j):
        at = bias_ref.at[:, cols_of(my_g)]
        return remote(at, at, c_send.at[j], c_recv.at[j], team(j), my_t)

    @pl.loop(1, members)
    def _(k):
        a_copy(k).start()

    @pl.loop(1, groups)
    def _(j):
        f_copy(0, j).start()

    @pl.loop(1, members)
    def _(k):
        b_copy(k).wait()

    def add(q, total):
        return total + bias_part[lax.rem(my_t - q + members, members)]

    bias_ref[:, cols_of(my_g)] = lax.fori_loop(1, members, add, bias_part[my_t])

    @pl.loop(1, groups)
    def _(j):
        c_copy(j).start()

    @pl.loop(1, members)
    def _(k):
        a_copy(k).wait_recv()

        @pl.loop(1, groups)
        def _(j):
            f_copy(k, j).start()

    @pl.loop(1, members)
    def _(k):
        a_copy(k).wait_send()

    @pl.loop(1, groups)
    def _(j):
        c_copy(j).wait()

        @pl.loop(0, members)
        def _(k):
            f_copy(k, j).wait()

    stores = [pltpu.make_async_copy(fin_ref, top_out, store_sem.at[1]),
              pltpu.make_async_copy(bias_ref, bias_out, store_sem.at[2])]
    for store in stores:
        store.start()
    for store in [logit_store] + stores:
        store.wait()


def finish_kernel(logit_in, top_in, bias_in, logit_ref, top_ref, bias_ref):
    logit_ref[...] = logit_in[...]
    members, slots, _ = top_in.shape
    for m in range(members):
        top_ref[m * slots : (m + 1) * slots, :] = top_in[m].astype(jnp.float32)
    bias_ref[...] = bias_in[...]


def fused_step(count, groups, members, ids, id_weights, d, table, slot_table, labels, weight, bias, out):
    samples, width = d.shape
    slots, vocab, _ = table.shape
    tables, hidden = weight.shape
    piece = hidden // groups
    per = 2 if members % 2 == 0 else 1
    hots = ids.shape[2] // tables
    own = slots * hots
    vmem = pl.BlockSpec(memory_space=pltpu.VMEM)
    hbm = pl.BlockSpec(memory_space=pltpu.HBM)
    f32, bf16 = jnp.float32, jnp.bfloat16
    dma = pltpu.SemaphoreType.DMA
    logit, top, side = pl.pallas_call(
        functools.partial(step_kernel, count, groups, members),
        out_shape=(
            jax.ShapeDtypeStruct(labels.shape, f32),
            jax.ShapeDtypeStruct((members, slots, hidden), bf16),
            jax.ShapeDtypeStruct((1, hidden), f32),
        ),
        in_specs=[hbm] * 10,
        out_specs=(hbm,) * 3,
        scratch_shapes=[
            pltpu.VMEM(ids.shape, jnp.int32),
            pltpu.VMEM(ids.shape, bf16),
            pltpu.SMEM((tables,), jnp.int32),
            pltpu.VMEM(table.shape, bf16),
            pltpu.VMEM((1, tables), jnp.int32),
            pltpu.VMEM(labels.shape, jnp.int32),
            pltpu.VMEM(weight.shape, bf16),
            pltpu.VMEM((1, hidden), f32),
            pltpu.VMEM((hidden // LANES, LANES), bf16),
            pltpu.VMEM(labels.shape, f32),
            pltpu.VMEM((1, hidden), f32),
            dma((10,)),
            dma((3,)),
            pltpu.VMEM((tables, hots, samples), f32),
            pltpu.VMEM((tables, hots, samples), f32),
            pltpu.VMEM((members, 2 * own, samples), bf16),
            pltpu.VMEM((members, slots, hidden), bf16),
            pltpu.VMEM((members, 2 * own, samples), bf16),
            pltpu.VMEM((members, samples, width), bf16),
            pltpu.VMEM((per, own, samples), jnp.int32),
            pltpu.VMEM((per, own, samples), f32),
            pltpu.VMEM((per, own, samples), f32),
            pltpu.VMEM((members, slots, samples), f32),
            pltpu.VMEM((tables, samples), f32),
            pltpu.VMEM((tables + 8, hidden), f32),
            pltpu.VMEM((samples, hidden), bf16),
            pltpu.VMEM((groups, tables + 8, piece), f32),
            pltpu.VMEM((tables + 8, piece), f32),
            pltpu.VMEM((members, slots, piece), f32),
            pltpu.VMEM((members, 1, piece), f32),
        ]
        + [dma((members,))] * 6 + [dma((groups,))] * 2 + [dma((members,))] * 6
        + [dma((groups, members))] * 2 + [dma((groups,))] * 2,
        compiler_params=pltpu.CompilerParams(collective_id=1, has_side_effects=True),
    )(ids, id_weights, slot_table, d, table, slot_table.reshape(1, -1), labels, weight, bias.reshape(1, -1),
      out.reshape(-1, LANES))
    return pl.pallas_call(
        finish_kernel,
        out_shape=(
            jax.ShapeDtypeStruct(labels.shape, f32),
            jax.ShapeDtypeStruct((tables, hidden), f32),
            jax.ShapeDtypeStruct((1, hidden), f32),
        ),
        in_specs=[vmem] * 3,
        out_specs=(vmem,) * 3,
    )(logit, top, side)


def per_device(
    sample_ids, id_weights, dense_features, click_labels, table_shards, slot_table, top_weight, top_bias, out_weight
):
    micro, local_batch, columns = sample_ids.shape
    tables = slot_table.shape[0]
    slots = table_shards.shape[0]
    width = dense_features.shape[2]
    hidden = top_weight.shape[1]
    members = lax.axis_size("tab")
    groups = lax.axis_size("grp")
    samples = micro * local_batch
    count = samples * groups * members
    logit, grad_top, grad_bias = fused_step(
        count, groups, members, sample_ids, id_weights, dense_features.reshape(samples, width), table_shards,
        slot_table, click_labels, top_weight, top_bias, out_weight
    )
    return (logit, grad_top, grad_bias.reshape(hidden))


def solution(mesh):
    return jax.shard_map(
        per_device,
        mesh=mesh,
        in_specs=(
            P(None, ("grp", "tab"), None),
            P(None, ("grp", "tab"), None),
            P(None, ("grp", "tab"), None),
            P(None, ("grp", "tab")),
            P("tab", None, None),
            P(),
            P(),
            P(),
            P(),
        ),
        out_specs=(P(None, ("grp", "tab")), P(), P()),
        check_vma=False,
    )
```

```python
import functools
import math

import jax
import jax.numpy as jnp
from jax import lax
from jax.experimental import pallas as pl
from jax.experimental.pallas import tpu as pltpu
from jax.sharding import PartitionSpec as P

HOTS = 8
LANES = 128
ROWS = 8
loss_scale = 32768.0
NT = (((1,), (1,)), ((), ()))
MESH = pl.DeviceIdType.MESH
TN = (((0,), (0,)), ((), ()))


def column_of(row):
    size = row.shape[1]
    eye = lax.broadcasted_iota(jnp.int32, (size, size), 0) == lax.broadcasted_iota(jnp.int32, (size, size), 1)
    return jnp.sum(jnp.where(eye, row, 0.0), axis=1, keepdims=True)


def pick_rows(block, spot):
    pick = lax.GatherDimensionNumbers(
        offset_dims=(), collapsed_slice_dims=(0,), start_index_map=(0,),
        operand_batching_dims=(1,), start_indices_batching_dims=(1,))
    return lax.gather(block, spot[..., None], pick, (1, 1), mode=lax.GatherScatterMode.PROMISE_IN_BOUNDS)


def choose_rows(tile_of, spot, bits, first, count):
    if count == 1:
        return pick_rows(tile_of(first), spot)
    half = 1 << ((count - 1).bit_length() - 1)
    low = choose_rows(tile_of, spot, bits, first, half)
    high = choose_rows(tile_of, spot, bits, first + half, count - half)
    return jnp.where(bits[half.bit_length() - 1], high, low)


def row_of(column):
    size = column.shape[0]
    eye = lax.broadcasted_iota(jnp.int32, (size, size), 0) == lax.broadcasted_iota(jnp.int32, (size, size), 1)
    return jnp.sum(jnp.where(eye, column, 0.0), axis=0, keepdims=True)


def step_kernel(count, groups, members, ids, weights, table_of, feats_in, shards, place_in, labels_in, top_in, bias_in, out_in,
                logit_out, top_out, bias_out,
                id_ref, weight_ref, table_ref, t_ref, place_ref, label_ref, w_ref, b_ref, o_ref, logit_ref, bias_ref,
                load_sem, store_sem, code_ref, turned_ref, x_ref, fin_ref, xs_ref, ds_ref, key_ref, acc_ref, mine_ref, back_ref,
                got_ref, grad_ref, slope_ref, group_ref, half_ref, send_ref, part_ref, bias_part,
                x_send, x_recv, d_send, d_recv, s_send, s_recv, g_send, g_recv, p_send, p_recv,
                b_send, b_recv, a_send, a_recv, f_send, f_recv, c_send, c_recv):
    my_g, my_t = lax.axis_index("grp"), lax.axis_index("tab")
    slots, vocab, width = t_ref.shape
    micro, local, columns = id_ref.shape
    own = x_ref.shape[1]
    samples = x_ref.shape[2]
    hots = own // slots
    blocks = vocab // LANES
    tiles = vocab // ROWS
    tables = got_ref.shape[0]
    hidden = w_ref.shape[1]
    piece = hidden // groups
    per = 2 if members % 2 == 0 else 1
    chunk = per * samples

    plane = max(n for n in range(1, members + 1) if members % n == 0 and n * n <= members)
    lines = members // plane
    even = members & (members - 1) == 0

    def move(k, way):
        if even:
            spot = 0
            for bit in range(members.bit_length() - 1):
                spot = spot + lax.rem(lax.div(my_t, 1 << bit) + lax.div(k, 1 << bit), 2) * (1 << bit)
            return spot
        line = lax.rem(lax.div(my_t, plane) + way * lax.div(k, plane) + lines, lines)
        return line * plane + lax.rem(lax.rem(my_t, plane) + way * lax.rem(k, plane) + plane, plane)

    def member(k):
        return move(jnp.int32(k), 1)

    def origin(k):
        return move(jnp.int32(k), -1)

    def team(k):
        return lax.rem(my_g + k, groups)

    def team_origin(k):
        return lax.rem(my_g - k + groups, groups)

    def remote(src, dst, send, recv, g, t):
        return pltpu.make_async_remote_copy(src_ref=src, dst_ref=dst, send_sem=send, recv_sem=recv,
                                            device_id={"grp": g, "tab": t}, device_id_type=MESH)

    def rows_of(t):
        return pl.ds(pl.multiple_of(t * slots, slots), slots)

    def cols_of(g):
        return pl.ds(pl.multiple_of(g * piece, LANES), piece)

    barrier = pltpu.get_barrier_semaphore()

    @pl.loop(1, members)
    def _(k):
        pl.semaphore_signal(barrier, inc=1, device_id={"grp": my_g, "tab": member(k)}, device_id_type=MESH)

    @pl.loop(1, groups)
    def _(k):
        pl.semaphore_signal(barrier, inc=1, device_id={"grp": team(k), "tab": my_t}, device_id_type=MESH)

    loads = [pltpu.make_async_copy(src, dst, load_sem.at[n]) for n, (src, dst) in enumerate((
        (table_of, table_ref), (ids, id_ref), (weights, weight_ref), (feats_in, ds_ref.at[0]), (shards, t_ref),
        (place_in, place_ref), (labels_in, label_ref), (top_in, w_ref), (bias_in, b_ref), (out_in, o_ref)))]
    for load in loads:
        load.start()
    for load in loads[:2]:
        load.wait()

    step = LANES // hots
    for c in range(columns // LANES):
        at = slice(c * LANES, (c + 1) * LANES)
        ids = id_ref[:, :, at].reshape(samples, LANES)
        code = jnp.left_shift(LANES + (ids & (LANES - 1)), jnp.right_shift(ids, LANES.bit_length() - 1))
        code = code.astype(jnp.float32).astype(jnp.bfloat16)
        code_ref[c * step : (c + 1) * step] = code.T.astype(jnp.float32).reshape(step, hots, samples)

    @pl.loop(0, members)
    def _(m):
        held = [code_ref[table_ref[m * slots + s]] for s in range(slots)]
        x_ref[m] = jnp.concatenate(held, axis=0).astype(jnp.bfloat16)

    loads[3].wait()
    pl.semaphore_wait(barrier, members + groups - 2)

    def x_copy(k):
        return remote(x_ref.at[member(k)], xs_ref.at[k], x_send, x_recv.at[k], my_g, member(k))

    def d_copy(k):
        return remote(ds_ref.at[0], ds_ref.at[k], d_send, d_recv.at[k], my_g, member(k))

    def pass_copy(line, k):
        at = line * plane + k
        return remote(ds_ref.at[line * plane], ds_ref.at[at], d_send, d_recv.at[at], my_g, member(k))

    def s_copy(k):
        return remote(mine_ref.at[k], back_ref.at[k], s_send, s_recv.at[k], my_g, origin(k))

    @pl.loop(1, lines)
    def _(line):
        d_copy(line * plane).start()

    @pl.loop(1, plane)
    def _(k):
        d_copy(k).start()

    @pl.loop(1, min(2 * per, members))
    def _(k):
        x_copy(k).start()

    @pl.loop(3 * per, members)
    def _(k):
        x_copy(k).start()

    @pl.loop(2 * per, min(3 * per, members))
    def _(k):
        x_copy(k).start()

    xs_ref[0] = x_ref[my_t]
    loads[2].wait()
    for c in range(columns // LANES):
        share = weight_ref[:, :, c * LANES : (c + 1) * LANES].reshape(samples, LANES)
        turned_ref[c * step : (c + 1) * step] = share.T.astype(jnp.float32).reshape(step, hots, samples)
    loads[4].wait()

    parts = 2 if vocab % (2 * ROWS) == 0 else 1
    unroll = 4 if slots % 4 == 0 else 1

    turns = members // per

    @pl.loop(0, turns)
    def _(turn):
        late = lax.div(turn + turns - 2, turns)
        i = (1 - late) * turn + late * (2 + lax.rem(turn - 1, turns - 2)) if turns > 2 else turn

        for e in range(per):
            @pl.when(lax.rem(per * i + e, plane) > 0)
            def _():
                d_copy(per * i + e).wait_recv()

            @pl.when(per * i + e > 0)
            def _():
                x_copy(per * i + e).wait_recv()

        for e in range(per):
            code = xs_ref[per * i + e].astype(jnp.float32)
            high = jnp.zeros(code.shape, jnp.int32)
            for k in range(1, blocks):
                high = high + (code >= float(LANES << k)).astype(jnp.int32)
            low = jnp.right_shift(code.astype(jnp.int32), high) & (LANES - 1)
            key_ref[e] = high * LANES + low

        def look(slot):
            feats = ds_ref[pl.ds(per * i, per)].reshape(chunk, width)
            size = vocab // parts
            products = [lax.dot_general(t_ref[slot, p * size : (p + 1) * size, :], feats, NT,
                                        preferred_element_type=jnp.float32) for p in range(parts)]
            at = pl.ds(pl.multiple_of(slot * hots, hots), hots)
            for e in range(per):
                key = key_ref[e, at, :]
                high = jnp.right_shift(key, ROWS.bit_length() - 1)
                bits = [(high & (1 << b)) != 0 for b in range((tiles - 1).bit_length())]

                def tile_of(v, e=e):
                    p, r = divmod(v * ROWS, size)
                    return products[p][r : r + ROWS, e * samples : (e + 1) * samples]

                acc_ref[e, at, :] = choose_rows(tile_of, key & (ROWS - 1), bits, 0, tiles)

        @pl.loop(0, slots // unroll)
        def _(q):
            line = turn * (slots // unroll) + q - max(slots // unroll, 2) + 2

            @pl.when((line > 0) & (line < lines))
            def _():
                d_copy(line * plane).wait_recv()

                @pl.loop(1, plane)
                def _(k):
                    pass_copy(line, k).start()

            for u in range(unroll):
                look(q * unroll + u)

        for e in range(per):
            mine_ref[per * i + e] = acc_ref[e].astype(jnp.bfloat16)

        for e in range(per):
            @pl.when(per * i + e > 0)
            def _():
                s_copy(per * i + e).start()

    back_ref[0] = mine_ref[0]

    @pl.loop(0, members)
    def _(n):
        k = lax.rem(n + 3 * per, members)

        @pl.when(k > 0)
        def _():
            s_copy(k).wait_recv()

        t = member(k)
        shares = jnp.concatenate([turned_ref[table_ref[t * slots + s]] for s in range(slots)], axis=0)
        total = jnp.sum((back_ref[k].astype(jnp.float32) * shares).reshape(slots, hots, samples), axis=1)
        got_ref[rows_of(t), :] = (total * (1.0 / math.sqrt(width))).astype(jnp.bfloat16).astype(jnp.float32)

    rest = pl.ds(1, members - 1)
    remote(ds_ref.at[rest], ds_ref.at[rest], d_send, d_recv.at[0], my_g, my_t).wait_send()
    remote(x_ref.at[rest], xs_ref.at[rest], x_send, x_recv.at[0], my_g, my_t).wait_send()
    remote(mine_ref.at[rest], back_ref.at[rest], s_send, s_recv.at[0], my_g, my_t).wait_send()

    for load in loads[5:]:
        load.wait()
    row = lax.broadcasted_iota(jnp.int32, (tables, tables), 0)
    placed = (place_ref[...] == row).astype(jnp.bfloat16)
    scores = jnp.dot(placed, got_ref[...].astype(jnp.bfloat16), preferred_element_type=jnp.float32)
    scores = scores.astype(jnp.bfloat16)
    pre = lax.dot_general(scores, w_ref[...], TN, preferred_element_type=jnp.float32) + b_ref[...]
    gate = jax.nn.sigmoid(pre)
    value = (pre * gate).astype(jnp.bfloat16).astype(jnp.float32)
    out = o_ref[...].astype(jnp.float32)
    out = jnp.concatenate([out[r : r + 1, :] for r in range(out.shape[0])], axis=1)
    logit = jnp.sum(value * out, axis=1, keepdims=True)
    logit_row = row_of(logit)
    for m in range(micro):
        logit_ref[m : m + 1, :] = logit_row[:, m * local : (m + 1) * local]
    logit_store = pltpu.make_async_copy(logit_ref, logit_out, store_sem.at[0])
    logit_store.start()
    labels = jnp.concatenate([label_ref[m : m + 1, :].astype(jnp.float32) for m in range(micro)], axis=1)
    delta = (jax.nn.sigmoid(logit) - column_of(labels)) * (loss_scale / count)
    slope = gate * (1.0 + pre * (1.0 - gate))
    slope_ref[...] = (delta * out * slope).astype(jnp.bfloat16)
    grad = slope_ref[...]
    grad_ref[pl.ds(tables, 8), :] = jnp.broadcast_to(
        jnp.sum(grad.astype(jnp.float32), axis=0, keepdims=True), (8, hidden))
    grad_ref[pl.ds(0, tables), :] = jnp.dot(scores, grad, preferred_element_type=jnp.float32)

    def g_copy(k):
        return remote(grad_ref.at[:, cols_of(team(k))], group_ref.at[k], g_send.at[k], g_recv.at[k], team(k), my_t)

    @pl.loop(1, groups)
    def _(k):
        g_copy(k).start()

    half_ref[...] = grad_ref[:, cols_of(my_g)]

    @pl.loop(1, groups)
    def _(k):
        g_copy(k).wait()
        half_ref[...] += group_ref[k]

    send_ref[...] = half_ref[0:tables].reshape(members, slots, piece).astype(jnp.bfloat16)

    def p_copy(k):
        return remote(send_ref.at[member(k)], part_ref.at[k], p_send, p_recv, my_g, member(k))

    def b_copy(k):
        return remote(half_ref.at[pl.ds(tables, 1), :], bias_part.at[k], b_send, b_recv, my_g, member(k))

    @pl.loop(1, members)
    def _(k):
        p_copy(k).start()

    @pl.loop(1, members)
    def _(k):
        b_copy(k).start()

    bias_part[0] = half_ref[tables : tables + 1, :]

    remote(send_ref.at[rest], part_ref.at[rest], p_send, p_recv, my_g, my_t).wait()

    whole = half_ref[rows_of(my_t), :]
    for k in range(1, members):
        whole = whole + part_ref[k].astype(jnp.float32)
    fin_ref[my_t, :, cols_of(my_g)] = whole.astype(jnp.bfloat16)

    def a_copy(k):
        at = fin_ref.at[my_t, :, cols_of(my_g)]
        return remote(at, at, a_send, a_recv, my_g, member(k))

    def f_copy(j):
        at = fin_ref.at[:, :, cols_of(my_g)]
        return remote(at, at, f_send.at[j], f_recv.at[j], team(j), my_t)

    def c_copy(j):
        at = bias_ref.at[:, cols_of(my_g)]
        return remote(at, at, c_send.at[j], c_recv.at[j], team(j), my_t)

    @pl.loop(1, members)
    def _(k):
        a_copy(k).start()

    remote(bias_part.at[rest], bias_part.at[rest], b_send, b_recv, my_g, my_t).wait()

    def add(q, total):
        return total + bias_part[origin(q)]

    bias_ref[:, cols_of(my_g)] = lax.fori_loop(1, members, add, bias_part[my_t])

    @pl.loop(1, groups)
    def _(j):
        c_copy(j).start()

    held = fin_ref.at[rest, :, cols_of(my_g)]
    remote(held, held, a_send, a_recv, my_g, my_t).wait()

    @pl.loop(1, groups)
    def _(j):
        f_copy(j).start()

    @pl.loop(1, groups)
    def _(j):
        c_copy(j).wait()
        f_copy(j).wait()

    stores = [pltpu.make_async_copy(fin_ref, top_out, store_sem.at[1]),
              pltpu.make_async_copy(bias_ref, bias_out, store_sem.at[2])]
    for store in stores:
        store.start()
    for store in [logit_store] + stores:
        store.wait()


def finish_kernel(logit_in, top_in, bias_in, logit_ref, top_ref, bias_ref):
    logit_ref[...] = logit_in[...]
    members, slots, _ = top_in.shape
    for m in range(members):
        top_ref[m * slots : (m + 1) * slots, :] = top_in[m].astype(jnp.float32)
    bias_ref[...] = bias_in[...]


def fused_step(count, groups, members, ids, id_weights, d, table, slot_table, labels, weight, bias, out):
    samples, width = d.shape
    slots, vocab, _ = table.shape
    tables, hidden = weight.shape
    piece = hidden // groups
    per = 2 if members % 2 == 0 else 1
    hots = ids.shape[2] // tables
    own = slots * hots
    vmem = pl.BlockSpec(memory_space=pltpu.VMEM)
    hbm = pl.BlockSpec(memory_space=pltpu.HBM)
    f32, bf16 = jnp.float32, jnp.bfloat16
    dma = pltpu.SemaphoreType.DMA
    logit, top, side = pl.pallas_call(
        functools.partial(step_kernel, count, groups, members),
        out_shape=(
            jax.ShapeDtypeStruct(labels.shape, f32),
            jax.ShapeDtypeStruct((members, slots, hidden), bf16),
            jax.ShapeDtypeStruct((1, hidden), f32),
        ),
        in_specs=[hbm] * 10,
        out_specs=(hbm,) * 3,
        scratch_shapes=[
            pltpu.VMEM(ids.shape, jnp.int32),
            pltpu.VMEM(ids.shape, bf16),
            pltpu.SMEM((tables,), jnp.int32),
            pltpu.VMEM(table.shape, bf16),
            pltpu.VMEM((1, tables), jnp.int32),
            pltpu.VMEM(labels.shape, jnp.int32),
            pltpu.VMEM(weight.shape, bf16),
            pltpu.VMEM((1, hidden), f32),
            pltpu.VMEM((hidden // LANES, LANES), bf16),
            pltpu.VMEM(labels.shape, f32),
            pltpu.VMEM((1, hidden), f32),
            dma((10,)),
            dma((3,)),
            pltpu.VMEM((tables, hots, samples), f32),
            pltpu.VMEM((tables, hots, samples), f32),
            pltpu.VMEM((members, own, samples), bf16),
            pltpu.VMEM((members, slots, hidden), bf16),
            pltpu.VMEM((members, own, samples), bf16),
            pltpu.VMEM((members, samples, width), bf16),
            pltpu.VMEM((per, own, samples), jnp.int32),
            pltpu.VMEM((per, own, samples), f32),
            pltpu.VMEM((members, own, samples), bf16),
            pltpu.VMEM((members, own, samples), bf16),
            pltpu.VMEM((tables, samples), f32),
            pltpu.VMEM((tables + 8, hidden), f32),
            pltpu.VMEM((samples, hidden), bf16),
            pltpu.VMEM((groups, tables + 8, piece), f32),
            pltpu.VMEM((tables + 8, piece), f32),
            pltpu.VMEM((members, slots, piece), bf16),
            pltpu.VMEM((members, slots, piece), bf16),
            pltpu.VMEM((members, 1, piece), f32),
        ]
        + [dma, dma((members,))] * 3 + [dma((groups,))] * 2 + [dma] * 6 + [dma((groups,))] * 4,
        compiler_params=pltpu.CompilerParams(collective_id=1, has_side_effects=True),
    )(ids, id_weights, slot_table, d, table, slot_table.reshape(1, -1), labels, weight, bias.reshape(1, -1),
      out.reshape(-1, LANES))
    return pl.pallas_call(
        finish_kernel,
        out_shape=(
            jax.ShapeDtypeStruct(labels.shape, f32),
            jax.ShapeDtypeStruct((tables, hidden), f32),
            jax.ShapeDtypeStruct((1, hidden), f32),
        ),
        in_specs=[vmem] * 3,
        out_specs=(vmem,) * 3,
    )(logit, top, side)


def per_device(
    sample_ids, id_weights, dense_features, click_labels, table_shards, slot_table, top_weight, top_bias, out_weight
):
    micro, local_batch, columns = sample_ids.shape
    tables = slot_table.shape[0]
    slots = table_shards.shape[0]
    width = dense_features.shape[2]
    hidden = top_weight.shape[1]
    members = lax.axis_size("tab")
    groups = lax.axis_size("grp")
    samples = micro * local_batch
    count = samples * groups * members
    logit, grad_top, grad_bias = fused_step(
        count, groups, members, sample_ids, id_weights, dense_features.reshape(samples, width), table_shards,
        slot_table, click_labels, top_weight, top_bias, out_weight
    )
    return (logit, grad_top, grad_bias.reshape(hidden))


def solution(mesh):
    return jax.shard_map(
        per_device,
        mesh=mesh,
        in_specs=(
            P(None, ("grp", "tab"), None),
            P(None, ("grp", "tab"), None),
            P(None, ("grp", "tab"), None),
            P(None, ("grp", "tab")),
            P("tab", None, None),
            P(),
            P(),
            P(),
            P(),
        ),
        out_specs=(P(None, ("grp", "tab")), P(), P()),
        check_vma=False,
    )
```

```python
import functools
import math

import jax
import jax.numpy as jnp
from jax import lax
from jax.experimental import pallas as pl
from jax.experimental.pallas import tpu as pltpu
from jax.sharding import PartitionSpec as P

HOTS = 8
LANES = 128
ROWS = 8
loss_scale = 32768.0
NT = (((1,), (1,)), ((), ()))
MESH = pl.DeviceIdType.MESH
TN = (((0,), (0,)), ((), ()))


def column_of(row):
    size = row.shape[1]
    eye = lax.broadcasted_iota(jnp.int32, (size, size), 0) == lax.broadcasted_iota(jnp.int32, (size, size), 1)
    return jnp.sum(jnp.where(eye, row, 0.0), axis=1, keepdims=True)


def pick_rows(block, spot):
    pick = lax.GatherDimensionNumbers(
        offset_dims=(), collapsed_slice_dims=(0,), start_index_map=(0,),
        operand_batching_dims=(1,), start_indices_batching_dims=(1,))
    return lax.gather(block, spot[..., None], pick, (1, 1), mode=lax.GatherScatterMode.PROMISE_IN_BOUNDS)


def choose_rows(tile_of, spot, bits, first, count):
    if count == 1:
        return pick_rows(tile_of(first), spot)
    half = 1 << ((count - 1).bit_length() - 1)
    low = choose_rows(tile_of, spot, bits, first, half)
    high = choose_rows(tile_of, spot, bits, first + half, count - half)
    return jnp.where(bits[half.bit_length() - 1], high, low)


def row_of(column):
    size = column.shape[0]
    eye = lax.broadcasted_iota(jnp.int32, (size, size), 0) == lax.broadcasted_iota(jnp.int32, (size, size), 1)
    return jnp.sum(jnp.where(eye, column, 0.0), axis=0, keepdims=True)


def step_kernel(count, groups, members, ids, weights, table_of, feats_in, shards, place_in, labels_in, top_in, bias_in, out_in,
                logit_out, top_out, bias_out,
                id_ref, weight_ref, table_ref, t_ref, place_ref, label_ref, w_ref, b_ref, o_ref, logit_ref, bias_ref,
                load_sem, store_sem, code_ref, turned_ref, x_ref, fin_ref, xs_ref, ds_ref, mine_ref, back_ref,
                got_ref, grad_ref, slope_ref, group_ref, half_ref, send_ref, part_ref, bias_part,
                x_send, x_recv, d_send, d_recv, s_send, s_recv, g_send, g_recv, p_send, p_recv,
                b_send, b_recv, a_send, a_recv, f_send, f_recv, c_send, c_recv):
    my_g, my_t = lax.axis_index("grp"), lax.axis_index("tab")
    slots, vocab, width = t_ref.shape
    micro, local, columns = id_ref.shape
    own = x_ref.shape[1]
    samples = x_ref.shape[2]
    hots = own // slots
    blocks = vocab // LANES
    tiles = vocab // ROWS
    tables = got_ref.shape[0]
    hidden = w_ref.shape[1]
    piece = hidden // groups
    per = 2 if members % 2 == 0 else 1
    chunk = per * samples

    plane = max(n for n in range(1, members + 1) if members % n == 0 and n * n <= members)
    lines = members // plane
    even = members & (members - 1) == 0

    flips = [(1 << bit) * (1 - 2 * lax.rem(lax.div(my_t, 1 << bit), 2)) for bit in range(members.bit_length() - 1)]

    def move(k, way):
        if even:
            spot = my_t
            for bit, flip in enumerate(flips):
                if isinstance(k, int):
                    spot = spot + flip if k & (1 << bit) else spot
                else:
                    spot = spot + flip * lax.rem(lax.div(k, 1 << bit), 2)
            return spot
        line = lax.rem(lax.div(my_t, plane) + way * lax.div(k, plane) + lines, lines)
        return line * plane + lax.rem(lax.rem(my_t, plane) + way * lax.rem(k, plane) + plane, plane)

    def member(k):
        return move(k if even else jnp.int32(k), 1)

    def origin(k):
        return move(k if even else jnp.int32(k), -1)

    def team(k):
        return lax.rem(my_g + k, groups)

    def team_origin(k):
        return lax.rem(my_g - k + groups, groups)

    def remote(src, dst, send, recv, g, t):
        return pltpu.make_async_remote_copy(src_ref=src, dst_ref=dst, send_sem=send, recv_sem=recv,
                                            device_id={"grp": g, "tab": t}, device_id_type=MESH)

    def rows_of(t):
        return pl.ds(pl.multiple_of(t * slots, slots), slots)

    def cols_of(g):
        return pl.ds(pl.multiple_of(g * piece, LANES), piece)

    loads = [pltpu.make_async_copy(src, dst, load_sem.at[n]) for n, (src, dst) in enumerate((
        (table_of, table_ref), (ids, id_ref), (weights, weight_ref), (feats_in, ds_ref.at[0]), (shards, t_ref),
        (place_in, place_ref), (labels_in, label_ref), (top_in, w_ref), (bias_in, b_ref), (out_in, o_ref)))]
    for load in loads[:2]:
        load.start()

    barrier = pltpu.get_barrier_semaphore()

    for k in range(members - 1, 0, -1):
        pl.semaphore_signal(barrier, inc=1, device_id={"grp": my_g, "tab": member(k)}, device_id_type=MESH)

    @pl.loop(1, groups)
    def _(k):
        pl.semaphore_signal(barrier, inc=1, device_id={"grp": team(k), "tab": my_t}, device_id_type=MESH)

    for load in loads[2:]:
        load.start()
    for load in loads[:2]:
        load.wait()

    step = LANES // hots
    for c in range(columns // LANES):
        at = slice(c * LANES, (c + 1) * LANES)
        ids = id_ref[:, :, at].reshape(samples, LANES)
        code = jnp.left_shift(LANES + (ids & (LANES - 1)), jnp.right_shift(ids, LANES.bit_length() - 1))
        code = code.astype(jnp.float32).astype(jnp.bfloat16)
        code_ref[c * step : (c + 1) * step] = code.T.astype(jnp.float32).reshape(step, hots, samples)

    @pl.loop(0, members)
    def _(m):
        held = [code_ref[table_ref[m * slots + s]] for s in range(slots)]
        x_ref[m] = jnp.concatenate(held, axis=0).astype(jnp.bfloat16)

    loads[3].wait()
    pl.semaphore_wait(barrier, members + groups - 2)

    def x_copy(k):
        return remote(x_ref.at[member(k)], xs_ref.at[k], x_send, x_recv.at[k], my_g, member(k))

    def d_copy(k):
        return remote(ds_ref.at[0], ds_ref.at[k], d_send, d_recv.at[k], my_g, member(k))

    def pass_copy(line, k):
        at = line * plane + k
        return remote(ds_ref.at[line * plane], ds_ref.at[at], d_send, d_recv.at[at], my_g, member(k))

    def s_copy(k):
        return remote(mine_ref.at[k], back_ref.at[k], s_send, s_recv.at[k], my_g, origin(k))

    near = min(2 * plane, members)

    def give(first, last):
        @pl.loop(first, last)
        def _(k):
            d_copy(k).start()
            x_copy(k).start()

    give(1, per)

    @pl.loop(2, lines)
    def _(line):
        d_copy(line * plane).start()

    give(per, min(2 * per, near))
    give(min(3 * per, near), near)
    give(min(2 * per, near), min(3 * per, near))

    xs_ref[0] = x_ref[my_t]
    loads[2].wait()
    for c in range(columns // LANES):
        share = weight_ref[:, :, c * LANES : (c + 1) * LANES].reshape(samples, LANES)
        turned_ref[c * step : (c + 1) * step] = share.T.astype(jnp.float32).reshape(step, hots, samples)
    loads[4].wait()

    parts = 2 if vocab % (2 * ROWS) == 0 else 1
    turns = members // per
    twin = 2 if slots % 2 == 0 else 1

    def pass_line(line):
        d_copy(line * plane).wait_recv()

        @pl.loop(1, plane)
        def _(k):
            pass_copy(line, k).start()

    def arrive(k):
        @pl.when((k < near) | (lax.rem(k, plane) > 0))
        def _():
            d_copy(k).wait_recv()

        x_copy(k).wait_recv()

    def look(i, first, last):
        feats = ds_ref[pl.ds(per * i, per)].reshape(chunk, width)
        size = vocab // parts
        for slot in range(first, last, twin):
            products = [[lax.dot_general(t_ref[slot + u, p * size : (p + 1) * size, :], feats, NT,
                                         preferred_element_type=jnp.float32) for p in range(parts)] for u in range(twin)]
            at = slice(slot * hots, (slot + twin) * hots)
            for e in range(per):
                code = xs_ref[per * i + e, at].astype(jnp.float32)
                high = jnp.zeros(code.shape, jnp.int32)
                for k in range(1, blocks):
                    high = high + (code >= float(LANES << k)).astype(jnp.int32)
                low = jnp.right_shift(code.astype(jnp.int32), high) & (LANES - 1)
                ids = high * LANES + low
                got = []
                for u in range(twin):
                    key = ids[u * hots : (u + 1) * hots]
                    tile = jnp.right_shift(key, ROWS.bit_length() - 1)
                    bits = [(tile & (1 << b)) != 0 for b in range((tiles - 1).bit_length())]

                    def tile_of(v, u=u, e=e):
                        p, r = divmod(v * ROWS, size)
                        return products[u][p][r : r + ROWS, e * samples : (e + 1) * samples]

                    got.append(choose_rows(tile_of, key & (ROWS - 1), bits, 0, tiles))
                mine_ref[per * i + e, at] = jnp.concatenate(got, axis=0).astype(jnp.bfloat16)

    for k in range(1, per):
        arrive(k)
    middle = slots // 2 // twin * twin
    look(0, 0, middle)
    if lines > 2:
        pass_line(2)

    @pl.loop(near, members)
    def _(k):
        x_copy(k).start()

    look(0, middle, slots)
    for k in range(1, per):
        s_copy(k).start()

    @pl.loop(1, turns)
    def _(turn):
        @pl.when(turn + 2 < lines)
        def _():
            pass_line(turn + 2)

        late = lax.div(turn + turns - 2, turns)
        i = (1 - late) * turn + late * (2 + lax.rem(turn - 1, turns - 2)) if turns > 2 else turn
        for e in range(per):
            arrive(per * i + e)
        look(i, 0, slots)
        for e in range(per):
            s_copy(per * i + e).start()

    back_ref[0] = mine_ref[0]

    @pl.loop(0, members)
    def _(n):
        k = lax.rem(n + 3 * per, members)

        @pl.when(k > 0)
        def _():
            s_copy(k).wait_recv()

        t = member(k)
        shares = jnp.concatenate([turned_ref[table_ref[t * slots + s]] for s in range(slots)], axis=0)
        total = jnp.sum((back_ref[k].astype(jnp.float32) * shares).reshape(slots, hots, samples), axis=1)
        got_ref[rows_of(t), :] = (total * (1.0 / math.sqrt(width))).astype(jnp.bfloat16).astype(jnp.float32)

    rest = pl.ds(1, members - 1)
    remote(ds_ref.at[rest], ds_ref.at[rest], d_send, d_recv.at[0], my_g, my_t).wait_send()
    remote(x_ref.at[rest], xs_ref.at[rest], x_send, x_recv.at[0], my_g, my_t).wait_send()
    remote(mine_ref.at[rest], back_ref.at[rest], s_send, s_recv.at[0], my_g, my_t).wait_send()

    for load in loads[5:]:
        load.wait()
    row = lax.broadcasted_iota(jnp.int32, (tables, tables), 0)
    placed = (place_ref[...] == row).astype(jnp.bfloat16)
    scores = jnp.dot(placed, got_ref[...].astype(jnp.bfloat16), preferred_element_type=jnp.float32)
    scores = scores.astype(jnp.bfloat16)
    pre = lax.dot_general(scores, w_ref[...], TN, preferred_element_type=jnp.float32) + b_ref[...]
    gate = jax.nn.sigmoid(pre)
    value = (pre * gate).astype(jnp.bfloat16).astype(jnp.float32)
    out = o_ref[...].astype(jnp.float32)
    out = jnp.concatenate([out[r : r + 1, :] for r in range(out.shape[0])], axis=1)
    logit = jnp.sum(value * out, axis=1, keepdims=True)
    logit_row = row_of(logit)
    for m in range(micro):
        logit_ref[m : m + 1, :] = logit_row[:, m * local : (m + 1) * local]
    logit_store = pltpu.make_async_copy(logit_ref, logit_out, store_sem.at[0])
    logit_store.start()
    labels = jnp.concatenate([label_ref[m : m + 1, :].astype(jnp.float32) for m in range(micro)], axis=1)
    delta = (jax.nn.sigmoid(logit) - column_of(labels)) * (loss_scale / count)
    slope = gate * (1.0 + pre * (1.0 - gate))
    slope_ref[...] = (delta * out * slope).astype(jnp.bfloat16)
    def g_copy(k):
        return remote(grad_ref.at[:, cols_of(team(k))], group_ref.at[k], g_send.at[k], g_recv.at[k], team(k), my_t)

    def gradient(g, into, at):
        grad = slope_ref[:, cols_of(g)]
        into[pl.ds(tables, 8), at] = jnp.broadcast_to(
            jnp.sum(grad.astype(jnp.float32), axis=0, keepdims=True), (8, piece))
        into[pl.ds(0, tables), at] = jnp.dot(scores, grad, preferred_element_type=jnp.float32)

    for k in range(1, groups):
        gradient(team(k), grad_ref, cols_of(team(k)))
        g_copy(k).start()

    gradient(my_g, half_ref, pl.ds(0, piece))

    @pl.loop(1, groups)
    def _(k):
        g_copy(k).wait()
        half_ref[...] += group_ref[k]

    send_ref[...] = half_ref[0:tables].reshape(members, slots, piece).astype(jnp.bfloat16)

    def p_copy(k):
        return remote(send_ref.at[member(k)], part_ref.at[k], p_send, p_recv, my_g, member(k))

    def b_copy(k):
        return remote(half_ref.at[pl.ds(tables, 1), :], bias_part.at[k], b_send, b_recv, my_g, member(k))

    @pl.loop(1, members)
    def _(k):
        p_copy(k).start()

    @pl.loop(1, members)
    def _(k):
        b_copy(k).start()

    bias_part[0] = half_ref[tables : tables + 1, :]

    remote(send_ref.at[rest], part_ref.at[rest], p_send, p_recv, my_g, my_t).wait()

    whole = half_ref[rows_of(my_t), :]
    for k in range(1, members):
        whole = whole + part_ref[k].astype(jnp.float32)
    fin_ref[my_t, :, cols_of(my_g)] = whole.astype(jnp.bfloat16)

    def a_copy(k):
        at = fin_ref.at[my_t, :, cols_of(my_g)]
        return remote(at, at, a_send, a_recv, my_g, member(k))

    def f_copy(j):
        return remote(fin_ref.at[:, :, cols_of(my_g)], top_out.at[:, :, cols_of(my_g)], f_send.at[j], f_recv.at[j],
                      team(j), my_t)

    def c_copy(j):
        return remote(bias_ref.at[:, cols_of(my_g)], bias_out.at[:, cols_of(my_g)], c_send.at[j], c_recv.at[j],
                      team(j), my_t)

    stores = [pltpu.make_async_copy(fin_ref.at[:, :, cols_of(my_g)], top_out.at[:, :, cols_of(my_g)], store_sem.at[1]),
              pltpu.make_async_copy(bias_ref.at[:, cols_of(my_g)], bias_out.at[:, cols_of(my_g)], store_sem.at[2])]

    @pl.loop(1, members)
    def _(k):
        a_copy(k).start()

    remote(bias_part.at[rest], bias_part.at[rest], b_send, b_recv, my_g, my_t).wait()

    def add(q, total):
        return total + bias_part[origin(q)]

    bias_ref[:, cols_of(my_g)] = lax.fori_loop(1, members, add, bias_part[my_t])

    for j in range(1, groups):
        c_copy(j).start()
    stores[1].start()

    held = fin_ref.at[rest, :, cols_of(my_g)]
    remote(held, held, a_send, a_recv, my_g, my_t).wait()

    for j in range(1, groups):
        f_copy(j).start()
    stores[0].start()

    for j in range(1, groups):
        c_copy(j).wait()
        f_copy(j).wait()
    for store in [logit_store] + stores:
        store.wait()


def finish_kernel(logit_in, top_in, bias_in, logit_ref, top_ref, bias_ref):
    logit_ref[...] = logit_in[...]
    members, slots, _ = top_in.shape
    for m in range(members):
        top_ref[m * slots : (m + 1) * slots, :] = top_in[m].astype(jnp.float32)
    bias_ref[...] = bias_in[...]


def fused_step(count, groups, members, ids, id_weights, d, table, slot_table, labels, weight, bias, out):
    samples, width = d.shape
    slots, vocab, _ = table.shape
    tables, hidden = weight.shape
    piece = hidden // groups
    per = 2 if members % 2 == 0 else 1
    hots = ids.shape[2] // tables
    own = slots * hots
    vmem = pl.BlockSpec(memory_space=pltpu.VMEM)
    hbm = pl.BlockSpec(memory_space=pltpu.HBM)
    f32, bf16 = jnp.float32, jnp.bfloat16
    dma = pltpu.SemaphoreType.DMA
    logit, top, side = pl.pallas_call(
        functools.partial(step_kernel, count, groups, members),
        out_shape=(
            jax.ShapeDtypeStruct(labels.shape, f32),
            jax.ShapeDtypeStruct((members, slots, hidden), bf16),
            jax.ShapeDtypeStruct((1, hidden), f32),
        ),
        in_specs=[hbm] * 10,
        out_specs=(hbm,) * 3,
        scratch_shapes=[
            pltpu.VMEM(ids.shape, jnp.int32),
            pltpu.VMEM(ids.shape, bf16),
            pltpu.SMEM((tables,), jnp.int32),
            pltpu.VMEM(table.shape, bf16),
            pltpu.VMEM((1, tables), jnp.int32),
            pltpu.VMEM(labels.shape, jnp.int32),
            pltpu.VMEM(weight.shape, bf16),
            pltpu.VMEM((1, hidden), f32),
            pltpu.VMEM((hidden // LANES, LANES), bf16),
            pltpu.VMEM(labels.shape, f32),
            pltpu.VMEM((1, hidden), f32),
            dma((10,)),
            dma((3,)),
            pltpu.VMEM((tables, hots, samples), f32),
            pltpu.VMEM((tables, hots, samples), f32),
            pltpu.VMEM((members, own, samples), bf16),
            pltpu.VMEM((members, slots, hidden), bf16),
            pltpu.VMEM((members, own, samples), bf16),
            pltpu.VMEM((members, samples, width), bf16),
            pltpu.VMEM((members, own, samples), bf16),
            pltpu.VMEM((members, own, samples), bf16),
            pltpu.VMEM((tables, samples), f32),
            pltpu.VMEM((tables + 8, hidden), f32),
            pltpu.VMEM((samples, hidden), bf16),
            pltpu.VMEM((groups, tables + 8, piece), f32),
            pltpu.VMEM((tables + 8, piece), f32),
            pltpu.VMEM((members, slots, piece), bf16),
            pltpu.VMEM((members, slots, piece), bf16),
            pltpu.VMEM((members, 1, piece), f32),
        ]
        + [dma, dma((members,))] * 3 + [dma((groups,))] * 2 + [dma] * 6 + [dma((groups,))] * 4,
        compiler_params=pltpu.CompilerParams(collective_id=1, has_side_effects=True),
    )(ids, id_weights, slot_table, d, table, slot_table.reshape(1, -1), labels, weight, bias.reshape(1, -1),
      out.reshape(-1, LANES))
    return pl.pallas_call(
        finish_kernel,
        out_shape=(
            jax.ShapeDtypeStruct(labels.shape, f32),
            jax.ShapeDtypeStruct((tables, hidden), f32),
            jax.ShapeDtypeStruct((1, hidden), f32),
        ),
        in_specs=[vmem] * 3,
        out_specs=(vmem,) * 3,
    )(logit, top, side)


def per_device(
    sample_ids, id_weights, dense_features, click_labels, table_shards, slot_table, top_weight, top_bias, out_weight
):
    micro, local_batch, columns = sample_ids.shape
    tables = slot_table.shape[0]
    slots = table_shards.shape[0]
    width = dense_features.shape[2]
    hidden = top_weight.shape[1]
    members = lax.axis_size("tab")
    groups = lax.axis_size("grp")
    samples = micro * local_batch
    count = samples * groups * members
    logit, grad_top, grad_bias = fused_step(
        count, groups, members, sample_ids, id_weights, dense_features.reshape(samples, width), table_shards,
        slot_table, click_labels, top_weight, top_bias, out_weight
    )
    return (logit, grad_top, grad_bias.reshape(hidden))


def solution(mesh):
    return jax.shard_map(
        per_device,
        mesh=mesh,
        in_specs=(
            P(None, ("grp", "tab"), None),
            P(None, ("grp", "tab"), None),
            P(None, ("grp", "tab"), None),
            P(None, ("grp", "tab")),
            P("tab", None, None),
            P(),
            P(),
            P(),
            P(),
        ),
        out_specs=(P(None, ("grp", "tab")), P(), P()),
        check_vma=False,
    )
```

```python
import functools
import math

import jax
import jax.numpy as jnp
from jax import lax
from jax.experimental import pallas as pl
from jax.experimental.pallas import tpu as pltpu
from jax.sharding import PartitionSpec as P

HOTS = 8
LANES = 128
ROWS = 8
loss_scale = 32768.0
NT = (((1,), (1,)), ((), ()))
MESH = pl.DeviceIdType.MESH
TN = (((0,), (0,)), ((), ()))


def column_of(row):
    size = row.shape[1]
    eye = lax.broadcasted_iota(jnp.int32, (size, size), 0) == lax.broadcasted_iota(jnp.int32, (size, size), 1)
    return jnp.sum(jnp.where(eye, row, 0.0), axis=1, keepdims=True)


def pick_rows(block, spot):
    pick = lax.GatherDimensionNumbers(
        offset_dims=(), collapsed_slice_dims=(0,), start_index_map=(0,),
        operand_batching_dims=(1,), start_indices_batching_dims=(1,))
    return lax.gather(block, spot[..., None], pick, (1, 1), mode=lax.GatherScatterMode.PROMISE_IN_BOUNDS)


def choose_rows(tile_of, spot, bits, first, count):
    if count == 1:
        return pick_rows(tile_of(first), spot)
    half = 1 << ((count - 1).bit_length() - 1)
    low = choose_rows(tile_of, spot, bits, first, half)
    high = choose_rows(tile_of, spot, bits, first + half, count - half)
    return jnp.where(bits[half.bit_length() - 1], high, low)


def row_of(column):
    size = column.shape[0]
    eye = lax.broadcasted_iota(jnp.int32, (size, size), 0) == lax.broadcasted_iota(jnp.int32, (size, size), 1)
    return jnp.sum(jnp.where(eye, column, 0.0), axis=0, keepdims=True)


def step_kernel(count, groups, members, ids, weights, table_of, feats_in, shards, place_in, labels_in, top_in, bias_in, out_in,
                logit_out, top_out, bias_out,
                id_ref, weight_ref, table_ref, t_ref, place_ref, label_ref, w_ref, b_ref, o_ref, logit_ref, bias_ref,
                load_sem, store_sem, code_ref, turned_ref, x_ref, fin_ref, xs_ref, ds_ref, mine_ref, back_ref,
                got_ref, grad_ref, slope_ref, group_ref, half_ref, send_ref, part_ref, bias_part,
                x_send, x_recv, d_send, d_recv, s_send, s_recv, g_send, g_recv, p_send, p_recv,
                b_send, b_recv, a_send, a_recv, f_send, f_recv, c_send, c_recv):
    my_g, my_t = lax.axis_index("grp"), lax.axis_index("tab")
    slots, vocab, width = t_ref.shape
    micro, local, columns = id_ref.shape
    own = x_ref.shape[1]
    samples = x_ref.shape[2]
    hots = own // slots
    blocks = vocab // LANES
    tiles = vocab // ROWS
    tables = got_ref.shape[0]
    hidden = w_ref.shape[1]
    piece = hidden // groups

    plane = max(n for n in range(1, members + 1) if members % n == 0 and n * n <= members)
    lines = members // plane
    flips = [(1 << bit) * (1 - 2 * lax.rem(lax.div(my_t, 1 << bit), 2)) for bit in range(members.bit_length() - 1)]

    def member(k):
        spot = my_t
        for bit, flip in enumerate(flips):
            if isinstance(k, int):
                spot = spot + flip if k & (1 << bit) else spot
            else:
                spot = spot + flip * lax.rem(lax.div(k, 1 << bit), 2)
        return spot

    def peer(j):
        if isinstance(j, int):
            return member(plane if j == members - 1 else j + (j >= plane))
        return member(j + lax.div(j + members - plane, members) - (members - plane) * lax.div(j + 1, members))

    def team(k):
        return lax.rem(my_g + k, groups)

    def team_origin(k):
        return lax.rem(my_g - k + groups, groups)

    def remote(src, dst, send, recv, g, t):
        return pltpu.make_async_remote_copy(src_ref=src, dst_ref=dst, send_sem=send, recv_sem=recv,
                                            device_id={"grp": g, "tab": t}, device_id_type=MESH)

    def rows_of(t):
        return pl.ds(pl.multiple_of(t * slots, slots), slots)

    def cols_of(g):
        return pl.ds(pl.multiple_of(g * piece, LANES), piece)

    loads = [pltpu.make_async_copy(src, dst, load_sem.at[n]) for n, (src, dst) in enumerate((
        (table_of, table_ref), (ids, id_ref), (weights, weight_ref), (feats_in, ds_ref.at[0]), (shards, t_ref),
        (place_in, place_ref), (labels_in, label_ref), (top_in, w_ref), (bias_in, b_ref), (out_in, o_ref)))]
    for load in loads[:2]:
        load.start()

    barrier = pltpu.get_barrier_semaphore()

    for k in range(members - 1, 0, -1):
        pl.semaphore_signal(barrier, inc=1, device_id={"grp": my_g, "tab": member(k)}, device_id_type=MESH)

    @pl.loop(1, groups)
    def _(k):
        pl.semaphore_signal(barrier, inc=1, device_id={"grp": team(k), "tab": my_t}, device_id_type=MESH)

    for load in loads[2:]:
        load.start()
    for load in loads[:2]:
        load.wait()

    step = LANES // hots
    for c in range(columns // LANES):
        at = slice(c * LANES, (c + 1) * LANES)
        ids = id_ref[:, :, at].reshape(samples, LANES)
        code = jnp.left_shift(LANES + (ids & (LANES - 1)), jnp.right_shift(ids, LANES.bit_length() - 1))
        code = code.astype(jnp.float32).astype(jnp.bfloat16)
        code_ref[c * step : (c + 1) * step] = code.T.astype(jnp.float32).reshape(step, hots, samples)

    @pl.loop(0, members)
    def _(m):
        held = [code_ref[table_ref[m * slots + s]] for s in range(slots)]
        x_ref[m] = jnp.concatenate(held, axis=0).astype(jnp.bfloat16)

    loads[3].wait()
    pl.semaphore_wait(barrier, members + groups - 2)

    def x_copy(j):
        return remote(x_ref.at[peer(j)], xs_ref.at[j], x_send, x_recv.at[j], my_g, peer(j))

    def d_copy(j):
        return remote(ds_ref.at[0], ds_ref.at[j], d_send, d_recv.at[j], my_g, peer(j))

    def pass_copy(line, k):
        at = line * plane + k - 1
        return remote(ds_ref.at[line * plane - 1], ds_ref.at[at], d_send, d_recv.at[at], my_g, member(k))

    def s_copy(j):
        return remote(mine_ref.at[j], back_ref.at[j], s_send, s_recv.at[j], my_g, peer(j))

    far = 2 * plane - 1
    last = members - 1

    def give(j):
        d_copy(j).start()
        x_copy(j).start()

    give(1)
    give(2)
    for line in range(2, lines):
        d_copy(line * plane - 1).start()
    for j in range(3, far):
        give(j)
    give(last)

    xs_ref[0] = x_ref[my_t]
    loads[4].wait()
    parts = 2 if vocab % (2 * ROWS) == 0 else 1
    size = vocab // parts
    pairs = (members - 2) // 2

    def pass_line(line):
        d_copy(line * plane - 1).wait_recv()
        for k in range(1, plane):
            pass_copy(line, k).start()

    def search(j, slot, tile_of):
        at = slice(slot * hots, (slot + 2) * hots)
        code = xs_ref[j, at].astype(jnp.float32)
        high = jnp.zeros(code.shape, jnp.int32)
        for k in range(1, blocks):
            high = high + (code >= float(LANES << k)).astype(jnp.int32)
        low = jnp.right_shift(code.astype(jnp.int32), high) & (LANES - 1)
        ids = high * LANES + low
        got = []
        for u in range(2):
            key = ids[u * hots : (u + 1) * hots]
            tile = jnp.right_shift(key, ROWS.bit_length() - 1)
            bits = [(tile & (1 << b)) != 0 for b in range((tiles - 1).bit_length())]
            got.append(choose_rows(functools.partial(tile_of, u), key & (ROWS - 1), bits, 0, tiles))
        mine_ref[j, at] = jnp.concatenate(got, axis=0).astype(jnp.bfloat16)

    def span(p):
        return slice(p * size, (p + 1) * size)

    def look_pair(j, first, end):
        feats = ds_ref[pl.ds(j, 2)].reshape(2 * samples, width)
        for slot in range(first, end, 2):
            products = [[lax.dot_general(t_ref[slot + u, span(p), :], feats, NT, preferred_element_type=jnp.float32)
                         for p in range(parts)] for u in range(2)]
            for e in range(2):
                def tile_of(u, v):
                    p, r = divmod(v * ROWS, size)
                    return products[u][p][r : r + ROWS, e * samples : (e + 1) * samples]

                search(j + e, slot, tile_of)

    def look_one(j):
        feats = ds_ref[j]
        none = jnp.zeros_like(feats)
        feats = jnp.concatenate([jnp.concatenate([feats, none], axis=1), jnp.concatenate([none, feats], axis=1)], axis=0)
        for slot in range(0, slots, 2):
            products = [lax.dot_general(jnp.concatenate([t_ref[slot, span(p), :], t_ref[slot + 1, span(p), :]], axis=1),
                                        feats, NT, preferred_element_type=jnp.float32) for p in range(parts)]

            def tile_of(u, v):
                p, r = divmod(v * ROWS, size)
                return products[p][r : r + ROWS, u * samples : (u + 1) * samples]

            search(j, slot, tile_of)

    look_one(0)
    back_ref[0] = mine_ref[0]
    loads[2].wait()
    for c in range(columns // LANES):
        share = weight_ref[:, :, c * LANES : (c + 1) * LANES].reshape(samples, LANES)
        turned_ref[c * step : (c + 1) * step] = share.T.astype(jnp.float32).reshape(step, hots, samples)

    for j in (1, 2):
        d_copy(j).wait_recv()
        x_copy(j).wait_recv()
    middle = slots // 4 * 2
    look_pair(1, 0, middle)
    if lines > 2:
        pass_line(2)
    for j in range(far, last):
        x_copy(j).start()
    look_pair(1, middle, slots)
    for j in (1, 2):
        s_copy(j).start()

    @pl.loop(1, pairs)
    def _(turn):
        @pl.when(turn + 2 < lines)
        def _():
            d_copy((turn + 2) * plane - 1).wait_recv()
            for k in range(1, plane):
                pass_copy(turn + 2, k).start()

        for e in range(2):
            j = 2 * turn + 1 + e

            @pl.when((j < far) | (lax.rem(j + 1, plane) > 0))
            def _():
                d_copy(j).wait_recv()

            x_copy(j).wait_recv()
        look_pair(2 * turn + 1, 0, slots)
        for e in range(2):
            s_copy(2 * turn + 1 + e).start()

    d_copy(last).wait_recv()
    x_copy(last).wait_recv()
    look_one(last)
    s_copy(last).start()

    @pl.loop(0, members)
    def _(j):
        @pl.when(j > 0)
        def _():
            s_copy(j).wait_recv()

        t = peer(j)
        shares = jnp.concatenate([turned_ref[table_ref[t * slots + s]] for s in range(slots)], axis=0)
        total = jnp.sum((back_ref[j].astype(jnp.float32) * shares).reshape(slots, hots, samples), axis=1)
        got_ref[rows_of(t), :] = (total * (1.0 / math.sqrt(width))).astype(jnp.bfloat16).astype(jnp.float32)

    rest = pl.ds(1, members - 1)
    remote(ds_ref.at[rest], ds_ref.at[rest], d_send, d_recv.at[0], my_g, my_t).wait_send()
    remote(x_ref.at[rest], xs_ref.at[rest], x_send, x_recv.at[0], my_g, my_t).wait_send()
    remote(mine_ref.at[rest], back_ref.at[rest], s_send, s_recv.at[0], my_g, my_t).wait_send()

    for load in loads[5:]:
        load.wait()
    row = lax.broadcasted_iota(jnp.int32, (tables, tables), 0)
    placed = (place_ref[...] == row).astype(jnp.bfloat16)
    scores = jnp.dot(placed, got_ref[...].astype(jnp.bfloat16), preferred_element_type=jnp.float32)
    scores = scores.astype(jnp.bfloat16)
    pre = lax.dot_general(scores, w_ref[...], TN, preferred_element_type=jnp.float32) + b_ref[...]
    gate = jax.nn.sigmoid(pre)
    value = (pre * gate).astype(jnp.bfloat16).astype(jnp.float32)
    out = o_ref[...].astype(jnp.float32)
    out = jnp.concatenate([out[r : r + 1, :] for r in range(out.shape[0])], axis=1)
    logit = jnp.sum(value * out, axis=1, keepdims=True)
    logit_row = row_of(logit)
    for m in range(micro):
        logit_ref[m : m + 1, :] = logit_row[:, m * local : (m + 1) * local]
    logit_store = pltpu.make_async_copy(logit_ref, logit_out, store_sem.at[0])
    logit_store.start()
    labels = jnp.concatenate([label_ref[m : m + 1, :].astype(jnp.float32) for m in range(micro)], axis=1)
    delta = (jax.nn.sigmoid(logit) - column_of(labels)) * (loss_scale / count)
    slope = gate * (1.0 + pre * (1.0 - gate))
    slope_ref[...] = (delta * out * slope).astype(jnp.bfloat16)
    def g_copy(k):
        return remote(grad_ref.at[:, cols_of(team(k))], group_ref.at[k], g_send.at[k], g_recv.at[k], team(k), my_t)

    def gradient(g, into, at):
        grad = slope_ref[:, cols_of(g)]
        into[pl.ds(tables, 8), at] = jnp.broadcast_to(
            jnp.sum(grad.astype(jnp.float32), axis=0, keepdims=True), (8, piece))
        into[pl.ds(0, tables), at] = jnp.dot(scores, grad, preferred_element_type=jnp.float32)

    for k in range(1, groups):
        gradient(team(k), grad_ref, cols_of(team(k)))
        g_copy(k).start()

    gradient(my_g, half_ref, pl.ds(0, piece))

    @pl.loop(1, groups)
    def _(k):
        g_copy(k).wait()
        half_ref[...] += group_ref[k]

    send_ref[...] = half_ref[0:tables].reshape(members, slots, piece).astype(jnp.bfloat16)

    def p_copy(k):
        return remote(send_ref.at[member(k)], part_ref.at[k], p_send, p_recv, my_g, member(k))

    def b_copy(k):
        return remote(half_ref.at[pl.ds(tables, 1), :], bias_part.at[k], b_send, b_recv, my_g, member(k))

    for k in range(last, 0, -1):
        p_copy(k).start()
    for k in range(last, 0, -1):
        b_copy(k).start()

    bias_part[0] = half_ref[tables : tables + 1, :]

    remote(send_ref.at[rest], part_ref.at[rest], p_send, p_recv, my_g, my_t).wait()

    whole = half_ref[rows_of(my_t), :]
    for k in range(1, members):
        whole = whole + part_ref[k].astype(jnp.float32)
    fin_ref[my_t, :, cols_of(my_g)] = whole.astype(jnp.bfloat16)

    def a_copy(k):
        at = fin_ref.at[my_t, :, cols_of(my_g)]
        return remote(at, at, a_send, a_recv, my_g, member(k))

    def f_copy(j):
        return remote(fin_ref.at[:, :, cols_of(my_g)], top_out.at[:, :, cols_of(my_g)], f_send.at[j], f_recv.at[j],
                      team(j), my_t)

    def c_copy(j):
        return remote(bias_ref.at[:, cols_of(my_g)], bias_out.at[:, cols_of(my_g)], c_send.at[j], c_recv.at[j],
                      team(j), my_t)

    stores = [pltpu.make_async_copy(fin_ref.at[:, :, cols_of(my_g)], top_out.at[:, :, cols_of(my_g)], store_sem.at[1]),
              pltpu.make_async_copy(bias_ref.at[:, cols_of(my_g)], bias_out.at[:, cols_of(my_g)], store_sem.at[2])]

    for k in range(last, 0, -1):
        a_copy(k).start()

    remote(bias_part.at[rest], bias_part.at[rest], b_send, b_recv, my_g, my_t).wait()

    def add(q, total):
        return total + bias_part[member(q)]

    bias_ref[:, cols_of(my_g)] = lax.fori_loop(1, members, add, bias_part[my_t])

    for j in range(1, groups):
        c_copy(j).start()
    stores[1].start()

    held = fin_ref.at[rest, :, cols_of(my_g)]
    remote(held, held, a_send, a_recv, my_g, my_t).wait()

    for j in range(1, groups):
        f_copy(j).start()
    stores[0].start()

    for j in range(1, groups):
        c_copy(j).wait()
        f_copy(j).wait()
    for store in [logit_store] + stores:
        store.wait()


def finish_kernel(logit_in, top_in, bias_in, logit_ref, top_ref, bias_ref):
    logit_ref[...] = logit_in[...]
    members, slots, _ = top_in.shape
    for m in range(members):
        top_ref[m * slots : (m + 1) * slots, :] = top_in[m].astype(jnp.float32)
    bias_ref[...] = bias_in[...]


def fused_step(count, groups, members, ids, id_weights, d, table, slot_table, labels, weight, bias, out):
    samples, width = d.shape
    slots, vocab, _ = table.shape
    tables, hidden = weight.shape
    piece = hidden // groups
    hots = ids.shape[2] // tables
    own = slots * hots
    vmem = pl.BlockSpec(memory_space=pltpu.VMEM)
    hbm = pl.BlockSpec(memory_space=pltpu.HBM)
    f32, bf16 = jnp.float32, jnp.bfloat16
    dma = pltpu.SemaphoreType.DMA
    logit, top, side = pl.pallas_call(
        functools.partial(step_kernel, count, groups, members),
        out_shape=(
            jax.ShapeDtypeStruct(labels.shape, f32),
            jax.ShapeDtypeStruct((members, slots, hidden), bf16),
            jax.ShapeDtypeStruct((1, hidden), f32),
        ),
        in_specs=[hbm] * 10,
        out_specs=(hbm,) * 3,
        scratch_shapes=[
            pltpu.VMEM(ids.shape, jnp.int32),
            pltpu.VMEM(ids.shape, bf16),
            pltpu.SMEM((tables,), jnp.int32),
            pltpu.VMEM(table.shape, bf16),
            pltpu.VMEM((1, tables), jnp.int32),
            pltpu.VMEM(labels.shape, jnp.int32),
            pltpu.VMEM(weight.shape, bf16),
            pltpu.VMEM((1, hidden), f32),
            pltpu.VMEM((hidden // LANES, LANES), bf16),
            pltpu.VMEM(labels.shape, f32),
            pltpu.VMEM((1, hidden), f32),
            dma((10,)),
            dma((3,)),
            pltpu.VMEM((tables, hots, samples), f32),
            pltpu.VMEM((tables, hots, samples), f32),
            pltpu.VMEM((members, own, samples), bf16),
            pltpu.VMEM((members, slots, hidden), bf16),
            pltpu.VMEM((members, own, samples), bf16),
            pltpu.VMEM((members, samples, width), bf16),
            pltpu.VMEM((members, own, samples), bf16),
            pltpu.VMEM((members, own, samples), bf16),
            pltpu.VMEM((tables, samples), f32),
            pltpu.VMEM((tables + 8, hidden), f32),
            pltpu.VMEM((samples, hidden), bf16),
            pltpu.VMEM((groups, tables + 8, piece), f32),
            pltpu.VMEM((tables + 8, piece), f32),
            pltpu.VMEM((members, slots, piece), bf16),
            pltpu.VMEM((members, slots, piece), bf16),
            pltpu.VMEM((members, 1, piece), f32),
        ]
        + [dma, dma((members,))] * 3 + [dma((groups,))] * 2 + [dma] * 6 + [dma((groups,))] * 4,
        compiler_params=pltpu.CompilerParams(collective_id=1, has_side_effects=True),
    )(ids, id_weights, slot_table, d, table, slot_table.reshape(1, -1), labels, weight, bias.reshape(1, -1),
      out.reshape(-1, LANES))
    return pl.pallas_call(
        finish_kernel,
        out_shape=(
            jax.ShapeDtypeStruct(labels.shape, f32),
            jax.ShapeDtypeStruct((tables, hidden), f32),
            jax.ShapeDtypeStruct((1, hidden), f32),
        ),
        in_specs=[vmem] * 3,
        out_specs=(vmem,) * 3,
    )(logit, top, side)


def per_device(
    sample_ids, id_weights, dense_features, click_labels, table_shards, slot_table, top_weight, top_bias, out_weight
):
    micro, local_batch, columns = sample_ids.shape
    tables = slot_table.shape[0]
    slots = table_shards.shape[0]
    width = dense_features.shape[2]
    hidden = top_weight.shape[1]
    members = lax.axis_size("tab")
    groups = lax.axis_size("grp")
    samples = micro * local_batch
    count = samples * groups * members
    logit, grad_top, grad_bias = fused_step(
        count, groups, members, sample_ids, id_weights, dense_features.reshape(samples, width), table_shards,
        slot_table, click_labels, top_weight, top_bias, out_weight
    )
    return (logit, grad_top, grad_bias.reshape(hidden))


def solution(mesh):
    return jax.shard_map(
        per_device,
        mesh=mesh,
        in_specs=(
            P(None, ("grp", "tab"), None),
            P(None, ("grp", "tab"), None),
            P(None, ("grp", "tab"), None),
            P(None, ("grp", "tab")),
            P("tab", None, None),
            P(),
            P(),
            P(),
            P(),
        ),
        out_specs=(P(None, ("grp", "tab")), P(), P()),
        check_vma=False,
    )
```

```python
import functools
import math

import jax
import jax.numpy as jnp
from jax import lax
from jax.experimental import pallas as pl
from jax.experimental.pallas import tpu as pltpu
from jax.sharding import PartitionSpec as P

HOTS = 8
LANES = 128
ROWS = 8
loss_scale = 32768.0
NT = (((1,), (1,)), ((), ()))
MESH = pl.DeviceIdType.MESH
TN = (((0,), (0,)), ((), ()))


def column_of(row):
    size = row.shape[1]
    eye = lax.broadcasted_iota(jnp.int32, (size, size), 0) == lax.broadcasted_iota(jnp.int32, (size, size), 1)
    return jnp.sum(jnp.where(eye, row, 0.0), axis=1, keepdims=True)


def pick_rows(block, spot):
    pick = lax.GatherDimensionNumbers(
        offset_dims=(), collapsed_slice_dims=(0,), start_index_map=(0,),
        operand_batching_dims=(1,), start_indices_batching_dims=(1,))
    return lax.gather(block, spot[..., None], pick, (1, 1), mode=lax.GatherScatterMode.PROMISE_IN_BOUNDS)


def choose_rows(tile_of, spot, bits, first, count):
    if count == 1:
        return pick_rows(tile_of(first), spot)
    half = 1 << ((count - 1).bit_length() - 1)
    low = choose_rows(tile_of, spot, bits, first, half)
    high = choose_rows(tile_of, spot, bits, first + half, count - half)
    return jnp.where(bits[half.bit_length() - 1], high, low)


def row_of(column):
    size = column.shape[0]
    eye = lax.broadcasted_iota(jnp.int32, (size, size), 0) == lax.broadcasted_iota(jnp.int32, (size, size), 1)
    return jnp.sum(jnp.where(eye, column, 0.0), axis=0, keepdims=True)


def step_kernel(count, groups, members, ids, weights, table_of, feats_in, shards, place_in, labels_in, top_in, bias_in, out_in,
                logit_out, top_out, bias_out,
                id_ref, weight_ref, table_ref, t_ref, place_ref, label_ref, w_ref, b_ref, o_ref, logit_ref, bias_ref,
                load_sem, store_sem, code_ref, turned_ref, x_ref, fin_ref, xs_ref, ds_ref, mine_ref, back_ref,
                got_ref, grad_ref, slope_ref, group_ref, half_ref, send_ref, part_ref, bias_part,
                x_send, x_recv, d_send, d_recv, s_send, s_recv, g_send, g_recv, p_send, p_recv,
                b_send, b_recv, a_send, a_recv, f_send, f_recv, c_send, c_recv):
    my_g, my_t = lax.axis_index("grp"), lax.axis_index("tab")
    slots, vocab, width = t_ref.shape
    micro, local, columns = id_ref.shape
    own = x_ref.shape[1]
    samples = x_ref.shape[2]
    hots = own // slots
    blocks = vocab // LANES
    tiles = vocab // ROWS
    tables = got_ref.shape[0]
    hidden = w_ref.shape[1]
    piece = hidden // groups

    plane = max(n for n in range(1, members + 1) if members % n == 0 and n * n <= members)
    lines = members // plane
    flips = [(1 << bit) * (1 - 2 * lax.rem(lax.div(my_t, 1 << bit), 2)) for bit in range(members.bit_length() - 1)]

    def member(k):
        spot = my_t
        for bit, flip in enumerate(flips):
            if isinstance(k, int):
                spot = spot + flip if k & (1 << bit) else spot
            else:
                spot = spot + flip * lax.rem(lax.div(k, 1 << bit), 2)
        return spot

    def peer(j):
        if isinstance(j, int):
            return member(plane if j == members - 1 else j + (j >= plane))
        return member(j + lax.div(j + members - plane, members) - (members - plane) * lax.div(j + 1, members))

    def team(k):
        return lax.rem(my_g + k, groups)

    def team_origin(k):
        return lax.rem(my_g - k + groups, groups)

    def remote(src, dst, send, recv, g, t):
        return pltpu.make_async_remote_copy(src_ref=src, dst_ref=dst, send_sem=send, recv_sem=recv,
                                            device_id={"grp": g, "tab": t}, device_id_type=MESH)

    def rows_of(t):
        return pl.ds(pl.multiple_of(t * slots, slots), slots)

    def cols_of(g):
        return pl.ds(pl.multiple_of(g * piece, LANES), piece)

    loads = [pltpu.make_async_copy(src, dst, load_sem.at[n]) for n, (src, dst) in enumerate((
        (table_of, table_ref), (ids, id_ref), (weights, weight_ref), (feats_in, ds_ref.at[0]), (shards, t_ref),
        (place_in, place_ref), (labels_in, label_ref), (top_in, w_ref), (bias_in, b_ref), (out_in, o_ref)))]
    for load in loads[:2]:
        load.start()

    barrier = pltpu.get_barrier_semaphore()

    for k in range(members - 1, 0, -1):
        pl.semaphore_signal(barrier, inc=1, device_id={"grp": my_g, "tab": member(k)}, device_id_type=MESH)

    @pl.loop(1, groups)
    def _(k):
        pl.semaphore_signal(barrier, inc=1, device_id={"grp": team(k), "tab": my_t}, device_id_type=MESH)

    for load in loads[2:]:
        load.start()
    for load in loads[:2]:
        load.wait()

    step = LANES // hots
    for c in range(columns // LANES):
        at = slice(c * LANES, (c + 1) * LANES)
        ids = id_ref[:, :, at].reshape(samples, LANES)
        code = jnp.left_shift(LANES + (ids & (LANES - 1)), jnp.right_shift(ids, LANES.bit_length() - 1))
        code = code.astype(jnp.float32).astype(jnp.bfloat16)
        code_ref[c * step : (c + 1) * step] = code.T.astype(jnp.float32).reshape(step, hots, samples)

    @pl.loop(0, members)
    def _(m):
        held = [code_ref[table_ref[m * slots + s]] for s in range(slots)]
        x_ref[m] = jnp.concatenate(held, axis=0).astype(jnp.bfloat16)

    loads[3].wait()
    pl.semaphore_wait(barrier, members + groups - 2)

    def x_copy(j):
        return remote(x_ref.at[peer(j)], xs_ref.at[j], x_send, x_recv.at[lax.div(j + 1, 2)], my_g, peer(j))

    def d_copy(j):
        return remote(ds_ref.at[0], ds_ref.at[j], d_send, d_recv.at[j], my_g, peer(j))

    def pass_copy(line, k):
        at = line * plane + k - 1
        return remote(ds_ref.at[line * plane - 1], ds_ref.at[at], d_send, d_recv.at[at], my_g, member(k))

    def s_copy(j):
        return remote(mine_ref.at[j], back_ref.at[j], s_send, s_recv.at[lax.div(j + 1, 2)], my_g, peer(j))

    far = 2 * plane - 1
    last = members - 1

    def give(j):
        d_copy(j).start()
        x_copy(j).start()

    give(1)
    give(2)
    for line in range(2, lines):
        d_copy(line * plane - 1).start()
    for j in range(3, far):
        give(j)
    give(last)

    xs_ref[0] = x_ref[my_t]
    loads[4].wait()
    parts = 2 if vocab % (2 * ROWS) == 0 else 1
    size = vocab // parts
    pairs = (members - 2) // 2

    def pass_line(line):
        d_copy(line * plane - 1).wait_recv()
        for k in range(1, plane):
            pass_copy(line, k).start()

    def search(j, slot, tile_of):
        at = slice(slot * hots, (slot + 2) * hots)
        code = xs_ref[j, at].astype(jnp.float32)
        high = jnp.zeros(code.shape, jnp.int32)
        for k in range(1, blocks):
            high = high + (code >= float(LANES << k)).astype(jnp.int32)
        low = jnp.right_shift(code.astype(jnp.int32), high) & (LANES - 1)
        ids = high * LANES + low
        got = []
        for u in range(2):
            key = ids[u * hots : (u + 1) * hots]
            tile = jnp.right_shift(key, ROWS.bit_length() - 1)
            bits = [(tile & (1 << b)) != 0 for b in range((tiles - 1).bit_length())]
            got.append(choose_rows(functools.partial(tile_of, u), key & (ROWS - 1), bits, 0, tiles))
        mine_ref[j, at] = jnp.concatenate(got, axis=0).astype(jnp.bfloat16)

    def span(p):
        return slice(p * size, (p + 1) * size)

    def look_pair(j, first, end):
        feats = ds_ref[pl.ds(j, 2)].reshape(2 * samples, width)
        for slot in range(first, end, 2):
            products = [[lax.dot_general(t_ref[slot + u, span(p), :], feats, NT, preferred_element_type=jnp.float32)
                         for p in range(parts)] for u in range(2)]
            for e in range(2):
                def tile_of(u, v):
                    p, r = divmod(v * ROWS, size)
                    return products[u][p][r : r + ROWS, e * samples : (e + 1) * samples]

                search(j + e, slot, tile_of)

    def look_one(j):
        feats = ds_ref[j]
        none = jnp.zeros_like(feats)
        feats = jnp.concatenate([jnp.concatenate([feats, none], axis=1), jnp.concatenate([none, feats], axis=1)], axis=0)
        for slot in range(0, slots, 2):
            products = [lax.dot_general(jnp.concatenate([t_ref[slot, span(p), :], t_ref[slot + 1, span(p), :]], axis=1),
                                        feats, NT, preferred_element_type=jnp.float32) for p in range(parts)]

            def tile_of(u, v):
                p, r = divmod(v * ROWS, size)
                return products[p][r : r + ROWS, u * samples : (u + 1) * samples]

            search(j, slot, tile_of)

    look_one(0)
    back_ref[0] = mine_ref[0]
    loads[2].wait()
    for c in range(columns // LANES):
        share = weight_ref[:, :, c * LANES : (c + 1) * LANES].reshape(samples, LANES)
        turned_ref[c * step : (c + 1) * step] = share.T.astype(jnp.float32).reshape(step, hots, samples)

    def pair_in(j):
        two = pl.ds(j, 2)
        remote(x_ref.at[two], xs_ref.at[two], x_send, x_recv.at[lax.div(j + 1, 2)], my_g, my_t).wait_recv()

    def pair_back(j):
        two = pl.ds(j, 2)
        remote(mine_ref.at[two], back_ref.at[two], s_send, s_recv.at[lax.div(j + 1, 2)], my_g, my_t).wait_recv()

    for j in (1, 2):
        d_copy(j).wait_recv()
    pair_in(1)
    middle = slots // 4 * 2
    look_pair(1, 0, middle)
    if lines > 2:
        pass_line(2)
    for j in range(far, last):
        x_copy(j).start()
    look_pair(1, middle, slots)
    for j in (1, 2):
        s_copy(j).start()

    @pl.loop(1, pairs)
    def _(turn):
        @pl.when(turn + 2 < lines)
        def _():
            d_copy((turn + 2) * plane - 1).wait_recv()
            for k in range(1, plane):
                pass_copy(turn + 2, k).start()

        for e in range(2):
            j = 2 * turn + 1 + e

            @pl.when((j < far) | (lax.rem(j + 1, plane) > 0))
            def _():
                d_copy(j).wait_recv()

        pair_in(2 * turn + 1)
        look_pair(2 * turn + 1, 0, slots)
        for e in range(2):
            s_copy(2 * turn + 1 + e).start()

    d_copy(last).wait_recv()
    x_copy(last).wait_recv()
    look_one(last)
    s_copy(last).start()

    def settle(j):
        t = peer(j)
        shares = jnp.concatenate([turned_ref[table_ref[t * slots + s]] for s in range(slots)], axis=0)
        total = jnp.sum((back_ref[j].astype(jnp.float32) * shares).reshape(slots, hots, samples), axis=1)
        got_ref[rows_of(t), :] = (total * (1.0 / math.sqrt(width))).astype(jnp.bfloat16).astype(jnp.float32)

    settle(0)

    @pl.loop(0, pairs)
    def _(turn):
        pair_back(2 * turn + 1)
        for e in range(2):
            settle(2 * turn + 1 + e)

    s_copy(last).wait_recv()
    settle(last)

    rest = pl.ds(1, members - 1)

    for load in loads[5:]:
        load.wait()
    row = lax.broadcasted_iota(jnp.int32, (tables, tables), 0)
    placed = (place_ref[...] == row).astype(jnp.bfloat16)
    scores = jnp.dot(placed, got_ref[...].astype(jnp.bfloat16), preferred_element_type=jnp.float32)
    scores = scores.astype(jnp.bfloat16)
    pre = lax.dot_general(scores, w_ref[...], TN, preferred_element_type=jnp.float32) + b_ref[...]
    gate = jax.nn.sigmoid(pre)
    value = (pre * gate).astype(jnp.bfloat16).astype(jnp.float32)
    out = o_ref[...].astype(jnp.float32)
    out = jnp.concatenate([out[r : r + 1, :] for r in range(out.shape[0])], axis=1)
    logit = jnp.sum(value * out, axis=1, keepdims=True)
    logit_row = row_of(logit)
    for m in range(micro):
        logit_ref[m : m + 1, :] = logit_row[:, m * local : (m + 1) * local]
    logit_store = pltpu.make_async_copy(logit_ref, logit_out, store_sem.at[0])
    logit_store.start()
    labels = jnp.concatenate([label_ref[m : m + 1, :].astype(jnp.float32) for m in range(micro)], axis=1)
    delta = (jax.nn.sigmoid(logit) - column_of(labels)) * (loss_scale / count)
    slope = gate * (1.0 + pre * (1.0 - gate))
    slope_ref[...] = (delta * out * slope).astype(jnp.bfloat16)
    def g_copy(k):
        return remote(grad_ref.at[:, cols_of(team(k))], group_ref.at[k], g_send.at[k], g_recv.at[k], team(k), my_t)

    def gradient(g, into, at):
        grad = slope_ref[:, cols_of(g)]
        side = into.shape[0] - tables
        into[pl.ds(tables, side), at] = jnp.broadcast_to(
            jnp.sum(grad.astype(jnp.float32), axis=0, keepdims=True), (side, piece)).astype(into.dtype)
        into[pl.ds(0, tables), at] = jnp.dot(scores, grad, preferred_element_type=jnp.float32).astype(into.dtype)

    for k in range(1, groups):
        gradient(team(k), grad_ref, cols_of(team(k)))
        g_copy(k).start()

    gradient(my_g, half_ref, pl.ds(0, piece))

    for k in range(1, groups):
        g_copy(k).wait_recv()
        half_ref[...] += group_ref[k, 0 : tables + 8].astype(jnp.float32)

    send_ref[...] = half_ref[0:tables].reshape(members, slots, piece).astype(jnp.bfloat16)

    def p_copy(k):
        return remote(send_ref.at[member(k)], part_ref.at[k], p_send, p_recv, my_g, member(k))

    def b_copy(k):
        return remote(half_ref.at[pl.ds(tables, 1), :], bias_part.at[k], b_send, b_recv, my_g, member(k))

    for k in range(last, 0, -1):
        p_copy(k).start()
    for k in range(last, 0, -1):
        b_copy(k).start()

    bias_part[0] = half_ref[tables : tables + 1, :]

    parts_in = remote(send_ref.at[rest], part_ref.at[rest], p_send, p_recv, my_g, my_t)
    parts_in.wait_recv()

    whole = half_ref[rows_of(my_t), :]
    for k in range(1, members):
        whole = whole + part_ref[k].astype(jnp.float32)
    fin_ref[my_t, :, cols_of(my_g)] = whole.astype(jnp.bfloat16)

    def a_copy(k):
        at = fin_ref.at[my_t, :, cols_of(my_g)]
        return remote(at, at, a_send, a_recv, my_g, member(k))

    def f_copy(j):
        return remote(fin_ref.at[:, :, cols_of(my_g)], top_out.at[:, :, cols_of(my_g)], f_send.at[j], f_recv.at[j],
                      team(j), my_t)

    def c_copy(j):
        return remote(bias_ref.at[:, cols_of(my_g)], bias_out.at[:, cols_of(my_g)], c_send.at[j], c_recv.at[j],
                      team(j), my_t)

    stores = [pltpu.make_async_copy(fin_ref.at[:, :, cols_of(my_g)], top_out.at[:, :, cols_of(my_g)], store_sem.at[1]),
              pltpu.make_async_copy(bias_ref.at[:, cols_of(my_g)], bias_out.at[:, cols_of(my_g)], store_sem.at[2])]

    for k in range(last, 0, -1):
        a_copy(k).start()

    sides_in = remote(bias_part.at[rest], bias_part.at[rest], b_send, b_recv, my_g, my_t)
    sides_in.wait_recv()

    def add(q, total):
        return total + bias_part[member(q)]

    bias_ref[:, cols_of(my_g)] = lax.fori_loop(1, members, add, bias_part[my_t])

    for j in range(1, groups):
        c_copy(j).start()
    stores[1].start()

    held = fin_ref.at[rest, :, cols_of(my_g)]
    rows_in = remote(held, held, a_send, a_recv, my_g, my_t)
    rows_in.wait_recv()

    for j in range(1, groups):
        f_copy(j).start()
    stores[0].start()

    remote(ds_ref.at[rest], ds_ref.at[rest], d_send, d_recv.at[0], my_g, my_t).wait_send()
    remote(x_ref.at[rest], xs_ref.at[rest], x_send, x_recv.at[0], my_g, my_t).wait_send()
    remote(mine_ref.at[rest], back_ref.at[rest], s_send, s_recv.at[0], my_g, my_t).wait_send()
    for k in range(1, groups):
        g_copy(k).wait_send()
    for done in (parts_in, sides_in, rows_in):
        done.wait_send()
    for j in range(1, groups):
        c_copy(j).wait()
        f_copy(j).wait()
    for store in [logit_store] + stores:
        store.wait()


def finish_kernel(logit_in, top_in, bias_in, logit_ref, top_ref, bias_ref):
    logit_ref[...] = logit_in[...]
    members, slots, _ = top_in.shape
    for m in range(members):
        top_ref[m * slots : (m + 1) * slots, :] = top_in[m].astype(jnp.float32)
    bias_ref[...] = bias_in[...]


def fused_step(count, groups, members, ids, id_weights, d, table, slot_table, labels, weight, bias, out):
    samples, width = d.shape
    slots, vocab, _ = table.shape
    tables, hidden = weight.shape
    piece = hidden // groups
    hots = ids.shape[2] // tables
    own = slots * hots
    vmem = pl.BlockSpec(memory_space=pltpu.VMEM)
    hbm = pl.BlockSpec(memory_space=pltpu.HBM)
    f32, bf16 = jnp.float32, jnp.bfloat16
    dma = pltpu.SemaphoreType.DMA
    logit, top, side = pl.pallas_call(
        functools.partial(step_kernel, count, groups, members),
        out_shape=(
            jax.ShapeDtypeStruct(labels.shape, f32),
            jax.ShapeDtypeStruct((members, slots, hidden), bf16),
            jax.ShapeDtypeStruct((1, hidden), f32),
        ),
        in_specs=[hbm] * 10,
        out_specs=(hbm,) * 3,
        scratch_shapes=[
            pltpu.VMEM(ids.shape, jnp.int32),
            pltpu.VMEM(ids.shape, bf16),
            pltpu.SMEM((tables,), jnp.int32),
            pltpu.VMEM(table.shape, bf16),
            pltpu.VMEM((1, tables), jnp.int32),
            pltpu.VMEM(labels.shape, jnp.int32),
            pltpu.VMEM(weight.shape, bf16),
            pltpu.VMEM((1, hidden), f32),
            pltpu.VMEM((hidden // LANES, LANES), bf16),
            pltpu.VMEM(labels.shape, f32),
            pltpu.VMEM((1, hidden), f32),
            dma((10,)),
            dma((3,)),
            pltpu.VMEM((tables, hots, samples), f32),
            pltpu.VMEM((tables, hots, samples), f32),
            pltpu.VMEM((members, own, samples), bf16),
            pltpu.VMEM((members, slots, hidden), bf16),
            pltpu.VMEM((members, own, samples), bf16),
            pltpu.VMEM((members, samples, width), bf16),
            pltpu.VMEM((members, own, samples), bf16),
            pltpu.VMEM((members, own, samples), bf16),
            pltpu.VMEM((tables, samples), f32),
            pltpu.VMEM((tables + 16, hidden), bf16),
            pltpu.VMEM((samples, hidden), bf16),
            pltpu.VMEM((groups, tables + 16, piece), bf16),
            pltpu.VMEM((tables + 8, piece), f32),
            pltpu.VMEM((members, slots, piece), bf16),
            pltpu.VMEM((members, slots, piece), bf16),
            pltpu.VMEM((members, 1, piece), f32),
        ]
        + [dma, dma((members // 2 + 1,)), dma, dma((members,)), dma, dma((members // 2 + 1,))] + [dma((groups,))] * 2 + [dma] * 6 + [dma((groups,))] * 4,
        compiler_params=pltpu.CompilerParams(collective_id=1, has_side_effects=True),
    )(ids, id_weights, slot_table, d, table, slot_table.reshape(1, -1), labels, weight, bias.reshape(1, -1),
      out.reshape(-1, LANES))
    return pl.pallas_call(
        finish_kernel,
        out_shape=(
            jax.ShapeDtypeStruct(labels.shape, f32),
            jax.ShapeDtypeStruct((tables, hidden), f32),
            jax.ShapeDtypeStruct((1, hidden), f32),
        ),
        in_specs=[vmem] * 3,
        out_specs=(vmem,) * 3,
    )(logit, top, side)


def per_device(
    sample_ids, id_weights, dense_features, click_labels, table_shards, slot_table, top_weight, top_bias, out_weight
):
    micro, local_batch, columns = sample_ids.shape
    tables = slot_table.shape[0]
    slots = table_shards.shape[0]
    width = dense_features.shape[2]
    hidden = top_weight.shape[1]
    members = lax.axis_size("tab")
    groups = lax.axis_size("grp")
    samples = micro * local_batch
    count = samples * groups * members
    logit, grad_top, grad_bias = fused_step(
        count, groups, members, sample_ids, id_weights, dense_features.reshape(samples, width), table_shards,
        slot_table, click_labels, top_weight, top_bias, out_weight
    )
    return (logit, grad_top, grad_bias.reshape(hidden))


def solution(mesh):
    return jax.shard_map(
        per_device,
        mesh=mesh,
        in_specs=(
            P(None, ("grp", "tab"), None),
            P(None, ("grp", "tab"), None),
            P(None, ("grp", "tab"), None),
            P(None, ("grp", "tab")),
            P("tab", None, None),
            P(),
            P(),
            P(),
            P(),
        ),
        out_specs=(P(None, ("grp", "tab")), P(), P()),
        check_vma=False,
    )
```

```python
import functools
import math

import jax
import jax.numpy as jnp
from jax import lax
from jax.experimental import pallas as pl
from jax.experimental.pallas import tpu as pltpu
from jax.sharding import PartitionSpec as P

HOTS = 8
LANES = 128
ROWS = 8
loss_scale = 32768.0
NT = (((1,), (1,)), ((), ()))
MESH = pl.DeviceIdType.MESH
TN = (((0,), (0,)), ((), ()))


def column_of(row):
    size = row.shape[1]
    eye = lax.broadcasted_iota(jnp.int32, (size, size), 0) == lax.broadcasted_iota(jnp.int32, (size, size), 1)
    return jnp.sum(jnp.where(eye, row, 0.0), axis=1, keepdims=True)


def pick_rows(block, spot):
    pick = lax.GatherDimensionNumbers(
        offset_dims=(), collapsed_slice_dims=(0,), start_index_map=(0,),
        operand_batching_dims=(1,), start_indices_batching_dims=(1,))
    return lax.gather(block, spot[..., None], pick, (1, 1), mode=lax.GatherScatterMode.PROMISE_IN_BOUNDS)


def choose_rows(tile_of, spot, bits, first, count):
    if count == 1:
        return pick_rows(tile_of(first), spot)
    half = 1 << ((count - 1).bit_length() - 1)
    low = choose_rows(tile_of, spot, bits, first, half)
    high = choose_rows(tile_of, spot, bits, first + half, count - half)
    return jnp.where(bits[half.bit_length() - 1], high, low)


def row_of(column):
    size = column.shape[0]
    eye = lax.broadcasted_iota(jnp.int32, (size, size), 0) == lax.broadcasted_iota(jnp.int32, (size, size), 1)
    return jnp.sum(jnp.where(eye, column, 0.0), axis=0, keepdims=True)


def step_kernel(count, groups, members, ids, weights, table_of, feats_in, shards, place_in, labels_in, top_in, bias_in, out_in,
                logit_out, top_out, bias_out,
                id_ref, weight_ref, table_ref, t_ref, place_ref, label_ref, w_ref, b_ref, o_ref, logit_ref, bias_ref,
                load_sem, store_sem, code_ref, turned_ref, x_ref, fin_ref, xs_ref, ds_ref, mine_ref, back_ref,
                got_ref, grad_ref, slope_ref, group_ref, half_ref, send_ref, part_ref, bias_part,
                x_send, x_recv, d_send, d_recv, s_send, s_recv, g_send, g_recv, p_send, p_recv,
                b_send, b_recv, a_send, a_recv, f_send, f_recv, c_send, c_recv):
    my_g, my_t = lax.axis_index("grp"), lax.axis_index("tab")
    slots, vocab, width = t_ref.shape
    micro, local, columns = id_ref.shape
    own = x_ref.shape[1]
    samples = x_ref.shape[2]
    hots = own // slots
    blocks = vocab // LANES
    tiles = vocab // ROWS
    tables = got_ref.shape[0]
    hidden = w_ref.shape[1]
    piece = hidden // groups

    plane = max(n for n in range(1, members + 1) if members % n == 0 and n * n <= members)
    lines = members // plane
    flips = [(1 << bit) * (1 - 2 * lax.rem(lax.div(my_t, 1 << bit), 2)) for bit in range(members.bit_length() - 1)]

    def member(k):
        spot = my_t
        for bit, flip in enumerate(flips):
            if isinstance(k, int):
                spot = spot + flip if k & (1 << bit) else spot
            else:
                spot = spot + flip * lax.rem(lax.div(k, 1 << bit), 2)
        return spot

    def peer(j):
        if isinstance(j, int):
            return member(plane if j == members - 1 else j + (j >= plane))
        return member(j + lax.div(j + members - plane, members) - (members - plane) * lax.div(j + 1, members))

    def team(k):
        return lax.rem(my_g + k, groups)

    def team_origin(k):
        return lax.rem(my_g - k + groups, groups)

    def remote(src, dst, send, recv, g, t):
        return pltpu.make_async_remote_copy(src_ref=src, dst_ref=dst, send_sem=send, recv_sem=recv,
                                            device_id={"grp": g, "tab": t}, device_id_type=MESH)

    def rows_of(t):
        return pl.ds(pl.multiple_of(t * slots, slots), slots)

    def cols_of(g):
        return pl.ds(pl.multiple_of(g * piece, LANES), piece)

    loads = [pltpu.make_async_copy(src, dst, load_sem.at[n]) for n, (src, dst) in enumerate((
        (table_of, table_ref), (ids, id_ref), (weights, weight_ref), (feats_in, ds_ref.at[0]), (shards, t_ref),
        (place_in, place_ref), (labels_in, label_ref), (top_in, w_ref), (bias_in, b_ref), (out_in, o_ref)))]
    for load in loads[:2]:
        load.start()

    barrier = pltpu.get_barrier_semaphore()

    for k in range(members - 1, 0, -1):
        pl.semaphore_signal(barrier, inc=1, device_id={"grp": my_g, "tab": member(k)}, device_id_type=MESH)

    @pl.loop(1, groups)
    def _(k):
        pl.semaphore_signal(barrier, inc=1, device_id={"grp": team(k), "tab": my_t}, device_id_type=MESH)

    for load in loads[2:]:
        load.start()
    for load in loads[:2]:
        load.wait()

    step = LANES // hots
    for c in range(columns // LANES):
        at = slice(c * LANES, (c + 1) * LANES)
        ids = id_ref[:, :, at].reshape(samples, LANES)
        code = jnp.left_shift(LANES + (ids & (LANES - 1)), jnp.right_shift(ids, LANES.bit_length() - 1))
        code = code.astype(jnp.float32).astype(jnp.bfloat16)
        code_ref[c * step : (c + 1) * step] = code.T.astype(jnp.float32).reshape(step, hots, samples)

    @pl.loop(0, members)
    def _(m):
        held = [code_ref[table_ref[m * slots + s]] for s in range(slots)]
        x_ref[m] = jnp.concatenate(held, axis=0).astype(jnp.bfloat16)

    loads[3].wait()
    pl.semaphore_wait(barrier, members + groups - 2)

    def x_copy(j):
        return remote(x_ref.at[peer(j)], xs_ref.at[j], x_send, x_recv.at[lax.div(j + 1, 2)], my_g, peer(j))

    def d_copy(j):
        return remote(ds_ref.at[0], ds_ref.at[j], d_send, d_recv.at[j], my_g, peer(j))

    def pass_copy(line, k):
        at = line * plane + k - 1
        return remote(ds_ref.at[line * plane - 1], ds_ref.at[at], d_send, d_recv.at[at], my_g, member(k))

    def s_copy(j):
        return remote(mine_ref.at[j], back_ref.at[j], s_send, s_recv.at[lax.div(j + 1, 2)], my_g, peer(j))

    far = 2 * plane - 1
    last = members - 1

    def give(j):
        d_copy(j).start()
        x_copy(j).start()

    give(1)
    give(2)
    for line in range(2, lines):
        d_copy(line * plane - 1).start()
    for j in range(3, far):
        give(j)
    give(last)

    xs_ref[0] = x_ref[my_t]
    loads[4].wait()
    parts = 2 if vocab % (2 * ROWS) == 0 else 1
    size = vocab // parts
    pairs = (members - 2) // 2
    turned = plane - 1

    def pair_of(turn):
        late = lax.div(turn + pairs - turned, pairs)
        return turn + late * (turned + lax.rem(turn + 1 - turned, pairs - turned) - turn)

    def pass_line(line):
        d_copy(line * plane - 1).wait_recv()
        for k in range(1, plane):
            pass_copy(line, k).start()

    def search(j, slot, tile_of):
        at = slice(slot * hots, (slot + 2) * hots)
        code = xs_ref[j, at].astype(jnp.float32)
        high = jnp.zeros(code.shape, jnp.int32)
        for k in range(1, blocks):
            high = high + (code >= float(LANES << k)).astype(jnp.int32)
        low = jnp.right_shift(code.astype(jnp.int32), high) & (LANES - 1)
        ids = high * LANES + low
        got = []
        for u in range(2):
            key = ids[u * hots : (u + 1) * hots]
            tile = jnp.right_shift(key, ROWS.bit_length() - 1)
            bits = [(tile & (1 << b)) != 0 for b in range((tiles - 1).bit_length())]
            got.append(choose_rows(functools.partial(tile_of, u), key & (ROWS - 1), bits, 0, tiles))
        mine_ref[j, at] = jnp.concatenate(got, axis=0).astype(jnp.bfloat16)

    def span(p):
        return slice(p * size, (p + 1) * size)

    def look_pair(j, first, end):
        feats = ds_ref[pl.ds(j, 2)].reshape(2 * samples, width)
        for slot in range(first, end, 2):
            products = [[lax.dot_general(t_ref[slot + u, span(p), :], feats, NT, preferred_element_type=jnp.float32)
                         for p in range(parts)] for u in range(2)]
            for e in range(2):
                def tile_of(u, v):
                    p, r = divmod(v * ROWS, size)
                    return products[u][p][r : r + ROWS, e * samples : (e + 1) * samples]

                search(j + e, slot, tile_of)

    def look_one(j):
        feats = ds_ref[j]
        none = jnp.zeros_like(feats)
        feats = jnp.concatenate([jnp.concatenate([feats, none], axis=1), jnp.concatenate([none, feats], axis=1)], axis=0)
        for slot in range(0, slots, 2):
            products = [lax.dot_general(jnp.concatenate([t_ref[slot, span(p), :], t_ref[slot + 1, span(p), :]], axis=1),
                                        feats, NT, preferred_element_type=jnp.float32) for p in range(parts)]

            def tile_of(u, v):
                p, r = divmod(v * ROWS, size)
                return products[p][r : r + ROWS, u * samples : (u + 1) * samples]

            search(j, slot, tile_of)

    look_one(0)
    back_ref[0] = mine_ref[0]
    loads[2].wait()
    for c in range(columns // LANES):
        share = weight_ref[:, :, c * LANES : (c + 1) * LANES].reshape(samples, LANES)
        turned_ref[c * step : (c + 1) * step] = share.T.astype(jnp.float32).reshape(step, hots, samples)

    def pair_in(j):
        two = pl.ds(j, 2)
        remote(x_ref.at[two], xs_ref.at[two], x_send, x_recv.at[lax.div(j + 1, 2)], my_g, my_t).wait_recv()

    def pair_back(j):
        two = pl.ds(j, 2)
        remote(mine_ref.at[two], back_ref.at[two], s_send, s_recv.at[lax.div(j + 1, 2)], my_g, my_t).wait_recv()

    for j in (1, 2):
        d_copy(j).wait_recv()
    pair_in(1)
    middle = slots // 4 * 2
    look_pair(1, 0, middle)
    if lines > 2:
        pass_line(2)
    for j in [*range(far + 2, last), far, far + 1]:
        x_copy(j).start()
    look_pair(1, middle, slots)
    for j in (1, 2):
        s_copy(j).start()

    @pl.loop(1, pairs)
    def _(turn):
        @pl.when(turn + 2 < lines)
        def _():
            d_copy((turn + 2) * plane - 1).wait_recv()
            for k in range(1, plane):
                pass_copy(turn + 2, k).start()

        i = pair_of(turn)
        for e in range(2):
            j = 2 * i + 1 + e

            @pl.when((j < far) | (lax.rem(j + 1, plane) > 0))
            def _():
                d_copy(j).wait_recv()

        pair_in(2 * i + 1)
        look_pair(2 * i + 1, 0, slots)
        for e in range(2):
            s_copy(2 * i + 1 + e).start()

    d_copy(last).wait_recv()
    x_copy(last).wait_recv()
    look_one(last)
    s_copy(last).start()

    def settle(j):
        t = peer(j)
        shares = jnp.concatenate([turned_ref[table_ref[t * slots + s]] for s in range(slots)], axis=0)
        total = jnp.sum((back_ref[j].astype(jnp.float32) * shares).reshape(slots, hots, samples), axis=1)
        got_ref[rows_of(t), :] = (total * (1.0 / math.sqrt(width))).astype(jnp.bfloat16).astype(jnp.float32)

    settle(0)

    @pl.loop(0, pairs)
    def _(turn):
        i = pair_of(turn)
        pair_back(2 * i + 1)
        for e in range(2):
            settle(2 * i + 1 + e)

    s_copy(last).wait_recv()
    settle(last)

    rest = pl.ds(1, members - 1)

    for load in loads[5:]:
        load.wait()
    row = lax.broadcasted_iota(jnp.int32, (tables, tables), 0)
    placed = (place_ref[...] == row).astype(jnp.bfloat16)
    scores = jnp.dot(placed, got_ref[...].astype(jnp.bfloat16), preferred_element_type=jnp.float32)
    scores = scores.astype(jnp.bfloat16)
    pre = lax.dot_general(scores, w_ref[...], TN, preferred_element_type=jnp.float32) + b_ref[...]
    gate = jax.nn.sigmoid(pre)
    value = (pre * gate).astype(jnp.bfloat16).astype(jnp.float32)
    out = o_ref[...].astype(jnp.float32)
    out = jnp.concatenate([out[r : r + 1, :] for r in range(out.shape[0])], axis=1)
    logit = jnp.sum(value * out, axis=1, keepdims=True)
    logit_row = row_of(logit)
    for m in range(micro):
        logit_ref[m : m + 1, :] = logit_row[:, m * local : (m + 1) * local]
    logit_store = pltpu.make_async_copy(logit_ref, logit_out, store_sem.at[0])
    logit_store.start()
    labels = jnp.concatenate([label_ref[m : m + 1, :].astype(jnp.float32) for m in range(micro)], axis=1)
    delta = (jax.nn.sigmoid(logit) - column_of(labels)) * (loss_scale / count)
    slope = gate * (1.0 + pre * (1.0 - gate))
    slope_ref[...] = (delta * out * slope).astype(jnp.bfloat16)
    def g_copy(k):
        return remote(grad_ref.at[:, cols_of(team(k))], group_ref.at[k], g_send.at[k], g_recv.at[k], team(k), my_t)

    def gradient(g, into, at):
        grad = slope_ref[:, cols_of(g)]
        side = into.shape[0] - tables
        into[pl.ds(tables, side), at] = jnp.broadcast_to(
            jnp.sum(grad.astype(jnp.float32), axis=0, keepdims=True), (side, piece)).astype(into.dtype)
        into[pl.ds(0, tables), at] = jnp.dot(scores, grad, preferred_element_type=jnp.float32).astype(into.dtype)

    for k in range(1, groups):
        gradient(team(k), grad_ref, cols_of(team(k)))
        g_copy(k).start()

    gradient(my_g, half_ref, pl.ds(0, piece))

    for k in range(1, groups):
        g_copy(k).wait_recv()
        half_ref[...] += group_ref[k, 0 : tables + 8].astype(jnp.float32)

    send_ref[...] = half_ref[0:tables].reshape(members, slots, piece).astype(jnp.bfloat16)

    def p_copy(k):
        return remote(send_ref.at[member(k)], part_ref.at[k], p_send, p_recv, my_g, member(k))

    def b_copy(k):
        return remote(half_ref.at[pl.ds(tables, 1), :], bias_part.at[k], b_send, b_recv, my_g, member(k))

    for k in range(last, 0, -1):
        p_copy(k).start()
    for k in range(last, 0, -1):
        b_copy(k).start()

    bias_part[0] = half_ref[tables : tables + 1, :]

    parts_in = remote(send_ref.at[rest], part_ref.at[rest], p_send, p_recv, my_g, my_t)
    parts_in.wait_recv()

    whole = half_ref[rows_of(my_t), :]
    for k in range(1, members):
        whole = whole + part_ref[k].astype(jnp.float32)
    fin_ref[my_t, :, cols_of(my_g)] = whole.astype(jnp.bfloat16)

    def a_copy(k):
        at = fin_ref.at[my_t, :, cols_of(my_g)]
        return remote(at, at, a_send, a_recv, my_g, member(k))

    def f_copy(j):
        return remote(fin_ref.at[:, :, cols_of(my_g)], top_out.at[:, :, cols_of(my_g)], f_send.at[j], f_recv.at[j],
                      team(j), my_t)

    def c_copy(j):
        return remote(bias_ref.at[:, cols_of(my_g)], bias_out.at[:, cols_of(my_g)], c_send.at[j], c_recv.at[j],
                      team(j), my_t)

    stores = [pltpu.make_async_copy(fin_ref.at[:, :, cols_of(my_g)], top_out.at[:, :, cols_of(my_g)], store_sem.at[1]),
              pltpu.make_async_copy(bias_ref.at[:, cols_of(my_g)], bias_out.at[:, cols_of(my_g)], store_sem.at[2])]

    for k in range(last, 0, -1):
        a_copy(k).start()

    sides_in = remote(bias_part.at[rest], bias_part.at[rest], b_send, b_recv, my_g, my_t)
    sides_in.wait_recv()

    def add(q, total):
        return total + bias_part[member(q)]

    bias_ref[:, cols_of(my_g)] = lax.fori_loop(1, members, add, bias_part[my_t])

    for j in range(1, groups):
        c_copy(j).start()
    stores[1].start()

    held = fin_ref.at[rest, :, cols_of(my_g)]
    rows_in = remote(held, held, a_send, a_recv, my_g, my_t)
    rows_in.wait_recv()

    for j in range(1, groups):
        f_copy(j).start()
    stores[0].start()

    remote(ds_ref.at[rest], ds_ref.at[rest], d_send, d_recv.at[0], my_g, my_t).wait_send()
    remote(x_ref.at[rest], xs_ref.at[rest], x_send, x_recv.at[0], my_g, my_t).wait_send()
    remote(mine_ref.at[rest], back_ref.at[rest], s_send, s_recv.at[0], my_g, my_t).wait_send()
    for k in range(1, groups):
        g_copy(k).wait_send()
    for done in (parts_in, sides_in, rows_in):
        done.wait_send()
    for j in range(1, groups):
        c_copy(j).wait()
        f_copy(j).wait()
    for store in [logit_store] + stores:
        store.wait()


def finish_kernel(logit_in, top_in, bias_in, logit_ref, top_ref, bias_ref):
    logit_ref[...] = logit_in[...]
    members, slots, _ = top_in.shape
    for m in range(members):
        top_ref[m * slots : (m + 1) * slots, :] = top_in[m].astype(jnp.float32)
    bias_ref[...] = bias_in[...]


def fused_step(count, groups, members, ids, id_weights, d, table, slot_table, labels, weight, bias, out):
    samples, width = d.shape
    slots, vocab, _ = table.shape
    tables, hidden = weight.shape
    piece = hidden // groups
    hots = ids.shape[2] // tables
    own = slots * hots
    vmem = pl.BlockSpec(memory_space=pltpu.VMEM)
    hbm = pl.BlockSpec(memory_space=pltpu.HBM)
    f32, bf16 = jnp.float32, jnp.bfloat16
    dma = pltpu.SemaphoreType.DMA
    logit, top, side = pl.pallas_call(
        functools.partial(step_kernel, count, groups, members),
        out_shape=(
            jax.ShapeDtypeStruct(labels.shape, f32),
            jax.ShapeDtypeStruct((members, slots, hidden), bf16),
            jax.ShapeDtypeStruct((1, hidden), f32),
        ),
        in_specs=[hbm] * 10,
        out_specs=(hbm,) * 3,
        scratch_shapes=[
            pltpu.VMEM(ids.shape, jnp.int32),
            pltpu.VMEM(ids.shape, bf16),
            pltpu.SMEM((tables,), jnp.int32),
            pltpu.VMEM(table.shape, bf16),
            pltpu.VMEM((1, tables), jnp.int32),
            pltpu.VMEM(labels.shape, jnp.int32),
            pltpu.VMEM(weight.shape, bf16),
            pltpu.VMEM((1, hidden), f32),
            pltpu.VMEM((hidden // LANES, LANES), bf16),
            pltpu.VMEM(labels.shape, f32),
            pltpu.VMEM((1, hidden), f32),
            dma((10,)),
            dma((3,)),
            pltpu.VMEM((tables, hots, samples), f32),
            pltpu.VMEM((tables, hots, samples), f32),
            pltpu.VMEM((members, own, samples), bf16),
            pltpu.VMEM((members, slots, hidden), bf16),
            pltpu.VMEM((members, own, samples), bf16),
            pltpu.VMEM((members, samples, width), bf16),
            pltpu.VMEM((members, own, samples), bf16),
            pltpu.VMEM((members, own, samples), bf16),
            pltpu.VMEM((tables, samples), f32),
            pltpu.VMEM((tables + 16, hidden), bf16),
            pltpu.VMEM((samples, hidden), bf16),
            pltpu.VMEM((groups, tables + 16, piece), bf16),
            pltpu.VMEM((tables + 8, piece), f32),
            pltpu.VMEM((members, slots, piece), bf16),
            pltpu.VMEM((members, slots, piece), bf16),
            pltpu.VMEM((members, 1, piece), f32),
        ]
        + [dma, dma((members // 2 + 1,)), dma, dma((members,)), dma, dma((members // 2 + 1,))] + [dma((groups,))] * 2 + [dma] * 6 + [dma((groups,))] * 4,
        compiler_params=pltpu.CompilerParams(collective_id=1, has_side_effects=True),
    )(ids, id_weights, slot_table, d, table, slot_table.reshape(1, -1), labels, weight, bias.reshape(1, -1),
      out.reshape(-1, LANES))
    return pl.pallas_call(
        finish_kernel,
        out_shape=(
            jax.ShapeDtypeStruct(labels.shape, f32),
            jax.ShapeDtypeStruct((tables, hidden), f32),
            jax.ShapeDtypeStruct((1, hidden), f32),
        ),
        in_specs=[vmem] * 3,
        out_specs=(vmem,) * 3,
    )(logit, top, side)


def per_device(
    sample_ids, id_weights, dense_features, click_labels, table_shards, slot_table, top_weight, top_bias, out_weight
):
    micro, local_batch, columns = sample_ids.shape
    tables = slot_table.shape[0]
    slots = table_shards.shape[0]
    width = dense_features.shape[2]
    hidden = top_weight.shape[1]
    members = lax.axis_size("tab")
    groups = lax.axis_size("grp")
    samples = micro * local_batch
    count = samples * groups * members
    logit, grad_top, grad_bias = fused_step(
        count, groups, members, sample_ids, id_weights, dense_features.reshape(samples, width), table_shards,
        slot_table, click_labels, top_weight, top_bias, out_weight
    )
    return (logit, grad_top, grad_bias.reshape(hidden))


def solution(mesh):
    return jax.shard_map(
        per_device,
        mesh=mesh,
        in_specs=(
            P(None, ("grp", "tab"), None),
            P(None, ("grp", "tab"), None),
            P(None, ("grp", "tab"), None),
            P(None, ("grp", "tab")),
            P("tab", None, None),
            P(),
            P(),
            P(),
            P(),
        ),
        out_specs=(P(None, ("grp", "tab")), P(), P()),
        check_vma=False,
    )
```

```python
import functools
import math

import jax
import jax.numpy as jnp
from jax import lax
from jax.experimental import pallas as pl
from jax.experimental.pallas import tpu as pltpu
from jax.sharding import PartitionSpec as P

HOTS = 8
LANES = 128
ROWS = 8
loss_scale = 32768.0
NT = (((1,), (1,)), ((), ()))
MESH = pl.DeviceIdType.MESH
TN = (((0,), (0,)), ((), ()))


def column_of(row):
    size = row.shape[1]
    eye = lax.broadcasted_iota(jnp.int32, (size, size), 0) == lax.broadcasted_iota(jnp.int32, (size, size), 1)
    return jnp.sum(jnp.where(eye, row, 0.0), axis=1, keepdims=True)


def pick_rows(block, spot):
    pick = lax.GatherDimensionNumbers(
        offset_dims=(), collapsed_slice_dims=(0,), start_index_map=(0,),
        operand_batching_dims=(1,), start_indices_batching_dims=(1,))
    return lax.gather(block, spot[..., None], pick, (1, 1), mode=lax.GatherScatterMode.PROMISE_IN_BOUNDS)


def choose_rows(tile_of, spot, bits, first, count):
    if count == 1:
        return pick_rows(tile_of(first), spot)
    half = 1 << ((count - 1).bit_length() - 1)
    low = choose_rows(tile_of, spot, bits, first, half)
    high = choose_rows(tile_of, spot, bits, first + half, count - half)
    return jnp.where(bits[half.bit_length() - 1], high, low)


def row_of(column):
    size = column.shape[0]
    eye = lax.broadcasted_iota(jnp.int32, (size, size), 0) == lax.broadcasted_iota(jnp.int32, (size, size), 1)
    return jnp.sum(jnp.where(eye, column, 0.0), axis=0, keepdims=True)


def step_kernel(count, groups, members, ids, weights, table_of, feats_in, shards, place_in, labels_in, top_in, bias_in, out_in,
                logit_out, top_out, bias_out,
                id_ref, weight_ref, table_ref, t_ref, place_ref, label_ref, w_ref, b_ref, o_ref, logit_ref, bias_ref,
                load_sem, store_sem, code_ref, turned_ref, x_ref, fin_ref, xs_ref, ds_ref, mine_ref, back_ref,
                got_ref, grad_ref, slope_ref, group_ref, half_ref, send_ref, part_ref, bias_part,
                x_send, x_recv, d_send, d_recv, s_send, s_recv, g_send, g_recv, p_send, p_recv,
                b_send, b_recv, a_send, a_recv, f_send, f_recv, c_send, c_recv):
    my_g, my_t = lax.axis_index("grp"), lax.axis_index("tab")
    slots, vocab, width = t_ref.shape
    micro, local, columns = id_ref.shape
    own = x_ref.shape[1]
    samples = x_ref.shape[2]
    hots = own // slots
    blocks = vocab // LANES
    tiles = vocab // ROWS
    tables = got_ref.shape[0]
    hidden = w_ref.shape[1]
    piece = hidden // groups

    plane = max(n for n in range(1, members + 1) if members % n == 0 and n * n <= members)
    lines = members // plane
    flips = [(1 << bit) * (1 - 2 * lax.rem(lax.div(my_t, 1 << bit), 2)) for bit in range(members.bit_length() - 1)]

    def member(k):
        spot = my_t
        for bit, flip in enumerate(flips):
            if isinstance(k, int):
                spot = spot + flip if k & (1 << bit) else spot
            else:
                spot = spot + flip * lax.rem(lax.div(k, 1 << bit), 2)
        return spot

    def peer(j):
        if isinstance(j, int):
            return member(plane if j == members - 1 else j + (j >= plane))
        return member(j + lax.div(j + members - plane, members) - (members - plane) * lax.div(j + 1, members))

    def team(k):
        return lax.rem(my_g + k, groups)

    def team_origin(k):
        return lax.rem(my_g - k + groups, groups)

    def remote(src, dst, send, recv, g, t):
        return pltpu.make_async_remote_copy(src_ref=src, dst_ref=dst, send_sem=send, recv_sem=recv,
                                            device_id={"grp": g, "tab": t}, device_id_type=MESH)

    def rows_of(t):
        return pl.ds(pl.multiple_of(t * slots, slots), slots)

    def cols_of(g):
        return pl.ds(pl.multiple_of(g * piece, LANES), piece)

    loads = [pltpu.make_async_copy(src, dst, load_sem.at[n]) for n, (src, dst) in enumerate((
        (table_of, table_ref), (ids, id_ref), (weights, weight_ref), (feats_in, ds_ref.at[0]), (shards, t_ref),
        (place_in, place_ref), (labels_in, label_ref), (top_in, w_ref), (bias_in, b_ref), (out_in, o_ref)))]
    for load in loads[:2]:
        load.start()

    barrier = pltpu.get_barrier_semaphore()

    for k in range(members - 1, 0, -1):
        pl.semaphore_signal(barrier, inc=1, device_id={"grp": my_g, "tab": member(k)}, device_id_type=MESH)

    @pl.loop(1, groups)
    def _(k):
        pl.semaphore_signal(barrier, inc=1, device_id={"grp": team(k), "tab": my_t}, device_id_type=MESH)

    last = members - 1
    lend = groups % 2 == 0
    odd = lax.rem(my_g, 2) if lend else 1
    seat = members - odd
    if lend:
        pl.semaphore_signal(barrier, inc=1, device_id={"grp": my_g + 1 - 2 * odd, "tab": peer(last)}, device_id_type=MESH)

    for load in loads[2:]:
        load.start()
    for load in loads[:2]:
        load.wait()

    step = LANES // hots
    for c in range(columns // LANES):
        at = slice(c * LANES, (c + 1) * LANES)
        ids = id_ref[:, :, at].reshape(samples, LANES)
        code = jnp.left_shift(LANES + (ids & (LANES - 1)), jnp.right_shift(ids, LANES.bit_length() - 1))
        code = code.astype(jnp.float32).astype(jnp.bfloat16)
        code_ref[c * step : (c + 1) * step] = code.T.astype(jnp.float32).reshape(step, hots, samples)

    @pl.loop(0, members)
    def _(m):
        held = [code_ref[table_ref[m * slots + s]] for s in range(slots)]
        x_ref[m] = jnp.concatenate(held, axis=0).astype(jnp.bfloat16)

    loads[3].wait()
    pl.semaphore_wait(barrier, members + groups - 2 + lend)

    def x_copy(j):
        return remote(x_ref.at[peer(j)], xs_ref.at[j], x_send, x_recv.at[lax.div(j + 1, 2)], my_g, peer(j))

    def d_copy(j):
        return remote(ds_ref.at[0], ds_ref.at[j], d_send, d_recv.at[j], my_g, peer(j))

    def pass_copy(line, k):
        at = line * plane + k - 1
        return remote(ds_ref.at[line * plane - 1], ds_ref.at[at], d_send, d_recv.at[at], my_g, member(k))

    def s_copy(j):
        return remote(mine_ref.at[j], back_ref.at[j], s_send, s_recv.at[lax.div(j + 1, 2)], my_g, peer(j))

    far = 2 * plane - 1

    def give(j):
        d_copy(j).start()
        x_copy(j).start()

    give(1)
    give(2)
    for line in range(2, lines):
        d_copy(line * plane - 1).start()
    for j in range(3, far):
        give(j)
    remote(ds_ref.at[0], ds_ref.at[seat], d_send, d_recv.at[seat], my_g + 1 - odd, peer(last)).start()
    remote(x_ref.at[peer(last)], xs_ref.at[seat], x_send, x_recv.at[members // 2 + 1 - odd], my_g + 1 - odd,
           peer(last)).start()

    xs_ref[0] = x_ref[my_t]
    loads[4].wait()
    parts = 2 if vocab % (2 * ROWS) == 0 else 1
    size = vocab // parts
    pairs = (members - 2) // 2
    turned = plane - 1

    def pair_of(turn):
        late = lax.div(turn + pairs - turned, pairs)
        return turn + late * (turned + lax.rem(turn + 1 - turned, pairs - turned) - turn)

    def pass_line(line):
        d_copy(line * plane - 1).wait_recv()
        for k in range(1, plane):
            pass_copy(line, k).start()

    def search(j, slot, tile_of):
        at = slice(slot * hots, (slot + 2) * hots)
        code = xs_ref[j, at].astype(jnp.float32)
        high = jnp.zeros(code.shape, jnp.int32)
        for k in range(1, blocks):
            high = high + (code >= float(LANES << k)).astype(jnp.int32)
        low = jnp.right_shift(code.astype(jnp.int32), high) & (LANES - 1)
        ids = high * LANES + low
        got = []
        for u in range(2):
            key = ids[u * hots : (u + 1) * hots]
            tile = jnp.right_shift(key, ROWS.bit_length() - 1)
            bits = [(tile & (1 << b)) != 0 for b in range((tiles - 1).bit_length())]
            got.append(choose_rows(functools.partial(tile_of, u), key & (ROWS - 1), bits, 0, tiles))
        mine_ref[j, at] = jnp.concatenate(got, axis=0).astype(jnp.bfloat16)

    def span(p):
        return slice(p * size, (p + 1) * size)

    def look_pair(j, first, end):
        feats = ds_ref[pl.ds(j, 2)].reshape(2 * samples, width)
        for slot in range(first, end, 2):
            products = [[lax.dot_general(t_ref[slot + u, span(p), :], feats, NT, preferred_element_type=jnp.float32)
                         for p in range(parts)] for u in range(2)]
            for e in range(2):
                def tile_of(u, v):
                    p, r = divmod(v * ROWS, size)
                    return products[u][p][r : r + ROWS, e * samples : (e + 1) * samples]

                search(j + e, slot, tile_of)

    def look_one(j):
        feats = ds_ref[j]
        none = jnp.zeros_like(feats)
        feats = jnp.concatenate([jnp.concatenate([feats, none], axis=1), jnp.concatenate([none, feats], axis=1)], axis=0)
        for slot in range(0, slots, 2):
            products = [lax.dot_general(jnp.concatenate([t_ref[slot, span(p), :], t_ref[slot + 1, span(p), :]], axis=1),
                                        feats, NT, preferred_element_type=jnp.float32) for p in range(parts)]

            def tile_of(u, v):
                p, r = divmod(v * ROWS, size)
                return products[p][r : r + ROWS, u * samples : (u + 1) * samples]

            search(j, slot, tile_of)

    look_one(0)
    back_ref[0] = mine_ref[0]
    loads[2].wait()
    for c in range(columns // LANES):
        share = weight_ref[:, :, c * LANES : (c + 1) * LANES].reshape(samples, LANES)
        turned_ref[c * step : (c + 1) * step] = share.T.astype(jnp.float32).reshape(step, hots, samples)

    def pair_in(j):
        two = pl.ds(j, 2)
        remote(x_ref.at[two], xs_ref.at[two], x_send, x_recv.at[lax.div(j + 1, 2)], my_g, my_t).wait_recv()

    def pair_back(j):
        two = pl.ds(j, 2)
        remote(mine_ref.at[two], back_ref.at[two], s_send, s_recv.at[lax.div(j + 1, 2)], my_g, my_t).wait_recv()

    for j in (1, 2):
        d_copy(j).wait_recv()
    pair_in(1)
    middle = slots // 4 * 2
    look_pair(1, 0, middle)
    if lines > 2:
        pass_line(2)
    for j in [*range(far + 2, last), far, far + 1]:
        x_copy(j).start()
    look_pair(1, middle, slots)
    for j in (1, 2):
        s_copy(j).start()

    @pl.loop(1, pairs)
    def _(turn):
        @pl.when(turn + 2 < lines)
        def _():
            d_copy((turn + 2) * plane - 1).wait_recv()
            for k in range(1, plane):
                pass_copy(turn + 2, k).start()

        i = pair_of(turn)
        for e in range(2):
            j = 2 * i + 1 + e

            @pl.when((j < far) | (lax.rem(j + 1, plane) > 0))
            def _():
                d_copy(j).wait_recv()

        pair_in(2 * i + 1)
        look_pair(2 * i + 1, 0, slots)
        for e in range(2):
            s_copy(2 * i + 1 + e).start()

    def extra(n):
        j = members - n
        remote(ds_ref.at[0], ds_ref.at[j], d_send, d_recv.at[j], my_g, my_t).wait_recv()
        remote(x_ref.at[0], xs_ref.at[j], x_send, x_recv.at[members // 2 + 1 - n], my_g, my_t).wait_recv()
        look_one(j)
        remote(mine_ref.at[j], back_ref.at[last], s_send, s_recv.at[members // 2], my_g - 1 + n, peer(last)).start()

    if lend:
        @pl.when(odd == 1)
        def _():
            @pl.loop(0, 2)
            def _(n):
                extra(n)
    else:
        extra(1)

    def settle(j):
        t = peer(j)
        shares = jnp.concatenate([turned_ref[table_ref[t * slots + s]] for s in range(slots)], axis=0)
        total = jnp.sum((back_ref[j].astype(jnp.float32) * shares).reshape(slots, hots, samples), axis=1)
        got_ref[rows_of(t), :] = (total * (1.0 / math.sqrt(width))).astype(jnp.bfloat16).astype(jnp.float32)

    settle(0)

    @pl.loop(0, pairs)
    def _(turn):
        i = pair_of(turn)
        pair_back(2 * i + 1)
        for e in range(2):
            settle(2 * i + 1 + e)

    s_copy(last).wait_recv()
    settle(last)

    rest = pl.ds(1, members - 1)

    for load in loads[5:]:
        load.wait()
    row = lax.broadcasted_iota(jnp.int32, (tables, tables), 0)
    placed = (place_ref[...] == row).astype(jnp.bfloat16)
    scores = jnp.dot(placed, got_ref[...].astype(jnp.bfloat16), preferred_element_type=jnp.float32)
    scores = scores.astype(jnp.bfloat16)
    pre = lax.dot_general(scores, w_ref[...], TN, preferred_element_type=jnp.float32) + b_ref[...]
    gate = jax.nn.sigmoid(pre)
    value = (pre * gate).astype(jnp.bfloat16).astype(jnp.float32)
    out = o_ref[...].astype(jnp.float32)
    out = jnp.concatenate([out[r : r + 1, :] for r in range(out.shape[0])], axis=1)
    logit = jnp.sum(value * out, axis=1, keepdims=True)
    logit_row = row_of(logit)
    for m in range(micro):
        logit_ref[m : m + 1, :] = logit_row[:, m * local : (m + 1) * local]
    logit_store = pltpu.make_async_copy(logit_ref, logit_out, store_sem.at[0])
    logit_store.start()
    labels = jnp.concatenate([label_ref[m : m + 1, :].astype(jnp.float32) for m in range(micro)], axis=1)
    delta = (jax.nn.sigmoid(logit) - column_of(labels)) * (loss_scale / count)
    slope = gate * (1.0 + pre * (1.0 - gate))
    slope_ref[...] = (delta * out * slope).astype(jnp.bfloat16)
    def g_copy(k):
        return remote(grad_ref.at[:, cols_of(team(k))], group_ref.at[k], g_send.at[k], g_recv.at[k], team(k), my_t)

    def gradient(g, into, at):
        grad = slope_ref[:, cols_of(g)]
        side = into.shape[0] - tables
        into[pl.ds(tables, side), at] = jnp.broadcast_to(
            jnp.sum(grad.astype(jnp.float32), axis=0, keepdims=True), (side, piece)).astype(into.dtype)
        into[pl.ds(0, tables), at] = jnp.dot(scores, grad, preferred_element_type=jnp.float32).astype(into.dtype)

    for k in range(1, groups):
        gradient(team(k), grad_ref, cols_of(team(k)))
        g_copy(k).start()

    gradient(my_g, half_ref, pl.ds(0, piece))

    for k in range(1, groups):
        g_copy(k).wait_recv()
        half_ref[...] += group_ref[k, 0 : tables + 8].astype(jnp.float32)

    send_ref[...] = half_ref[0:tables].reshape(members, slots, piece).astype(jnp.bfloat16)

    def p_copy(k):
        return remote(send_ref.at[member(k)], part_ref.at[k], p_send, p_recv, my_g, member(k))

    def b_copy(k):
        return remote(half_ref.at[pl.ds(tables, 1), :], bias_part.at[k], b_send, b_recv, my_g, member(k))

    for k in range(last, 0, -1):
        p_copy(k).start()
    for k in range(last, 0, -1):
        b_copy(k).start()

    bias_part[0] = half_ref[tables : tables + 1, :]

    parts_in = remote(send_ref.at[rest], part_ref.at[rest], p_send, p_recv, my_g, my_t)
    parts_in.wait_recv()

    whole = half_ref[rows_of(my_t), :]
    for k in range(1, members):
        whole = whole + part_ref[k].astype(jnp.float32)
    fin_ref[my_t, :, cols_of(my_g)] = whole.astype(jnp.bfloat16)

    def a_copy(k):
        at = fin_ref.at[my_t, :, cols_of(my_g)]
        return remote(at, at, a_send, a_recv, my_g, member(k))

    def f_copy(j):
        return remote(fin_ref.at[:, :, cols_of(my_g)], top_out.at[:, :, cols_of(my_g)], f_send.at[j], f_recv.at[j],
                      team(j), my_t)

    def c_copy(j):
        return remote(bias_ref.at[:, cols_of(my_g)], bias_out.at[:, cols_of(my_g)], c_send.at[j], c_recv.at[j],
                      team(j), my_t)

    stores = [pltpu.make_async_copy(fin_ref.at[:, :, cols_of(my_g)], top_out.at[:, :, cols_of(my_g)], store_sem.at[1]),
              pltpu.make_async_copy(bias_ref.at[:, cols_of(my_g)], bias_out.at[:, cols_of(my_g)], store_sem.at[2])]

    for k in range(last, 0, -1):
        a_copy(k).start()

    sides_in = remote(bias_part.at[rest], bias_part.at[rest], b_send, b_recv, my_g, my_t)
    sides_in.wait_recv()

    def add(q, total):
        return total + bias_part[member(q)]

    bias_ref[:, cols_of(my_g)] = lax.fori_loop(1, members, add, bias_part[my_t])

    for j in range(1, groups):
        c_copy(j).start()
    stores[1].start()

    held = fin_ref.at[rest, :, cols_of(my_g)]
    rows_in = remote(held, held, a_send, a_recv, my_g, my_t)
    rows_in.wait_recv()

    for j in range(1, groups):
        f_copy(j).start()
    stores[0].start()

    remote(ds_ref.at[rest], ds_ref.at[rest], d_send, d_recv.at[0], my_g, my_t).wait_send()
    remote(x_ref.at[rest], xs_ref.at[rest], x_send, x_recv.at[0], my_g, my_t).wait_send()
    if lend:
        @pl.when(odd == 1)
        def _():
            both = pl.ds(1, members)
            remote(mine_ref.at[both], mine_ref.at[both], s_send, s_recv.at[0], my_g, my_t).wait_send()

        @pl.when(odd == 0)
        def _():
            most = pl.ds(1, members - 2)
            remote(mine_ref.at[most], mine_ref.at[most], s_send, s_recv.at[0], my_g, my_t).wait_send()
    else:
        remote(mine_ref.at[rest], back_ref.at[rest], s_send, s_recv.at[0], my_g, my_t).wait_send()
    for k in range(1, groups):
        g_copy(k).wait_send()
    for done in (parts_in, sides_in, rows_in):
        done.wait_send()
    for j in range(1, groups):
        c_copy(j).wait()
        f_copy(j).wait()
    for store in [logit_store] + stores:
        store.wait()


def finish_kernel(logit_in, top_in, bias_in, logit_ref, top_ref, bias_ref):
    logit_ref[...] = logit_in[...]
    members, slots, _ = top_in.shape
    for m in range(members):
        top_ref[m * slots : (m + 1) * slots, :] = top_in[m].astype(jnp.float32)
    bias_ref[...] = bias_in[...]


def fused_step(count, groups, members, ids, id_weights, d, table, slot_table, labels, weight, bias, out):
    samples, width = d.shape
    slots, vocab, _ = table.shape
    tables, hidden = weight.shape
    piece = hidden // groups
    hots = ids.shape[2] // tables
    own = slots * hots
    vmem = pl.BlockSpec(memory_space=pltpu.VMEM)
    hbm = pl.BlockSpec(memory_space=pltpu.HBM)
    f32, bf16 = jnp.float32, jnp.bfloat16
    dma = pltpu.SemaphoreType.DMA
    logit, top, side = pl.pallas_call(
        functools.partial(step_kernel, count, groups, members),
        out_shape=(
            jax.ShapeDtypeStruct(labels.shape, f32),
            jax.ShapeDtypeStruct((members, slots, hidden), bf16),
            jax.ShapeDtypeStruct((1, hidden), f32),
        ),
        in_specs=[hbm] * 10,
        out_specs=(hbm,) * 3,
        scratch_shapes=[
            pltpu.VMEM(ids.shape, jnp.int32),
            pltpu.VMEM(ids.shape, bf16),
            pltpu.SMEM((tables,), jnp.int32),
            pltpu.VMEM(table.shape, bf16),
            pltpu.VMEM((1, tables), jnp.int32),
            pltpu.VMEM(labels.shape, jnp.int32),
            pltpu.VMEM(weight.shape, bf16),
            pltpu.VMEM((1, hidden), f32),
            pltpu.VMEM((hidden // LANES, LANES), bf16),
            pltpu.VMEM(labels.shape, f32),
            pltpu.VMEM((1, hidden), f32),
            dma((10,)),
            dma((3,)),
            pltpu.VMEM((tables, hots, samples), f32),
            pltpu.VMEM((tables, hots, samples), f32),
            pltpu.VMEM((members, own, samples), bf16),
            pltpu.VMEM((members, slots, hidden), bf16),
            pltpu.VMEM((members + 1, own, samples), bf16),
            pltpu.VMEM((members + 1, samples, width), bf16),
            pltpu.VMEM((members + 1, own, samples), bf16),
            pltpu.VMEM((members, own, samples), bf16),
            pltpu.VMEM((tables, samples), f32),
            pltpu.VMEM((tables + 16, hidden), bf16),
            pltpu.VMEM((samples, hidden), bf16),
            pltpu.VMEM((groups, tables + 16, piece), bf16),
            pltpu.VMEM((tables + 8, piece), f32),
            pltpu.VMEM((members, slots, piece), bf16),
            pltpu.VMEM((members, slots, piece), bf16),
            pltpu.VMEM((members, 1, piece), f32),
        ]
        + [dma, dma((members // 2 + 2,)), dma, dma((members + 1,)), dma, dma((members // 2 + 1,))] + [dma((groups,))] * 2 + [dma] * 6 + [dma((groups,))] * 4,
        compiler_params=pltpu.CompilerParams(collective_id=1, has_side_effects=True),
    )(ids, id_weights, slot_table, d, table, slot_table.reshape(1, -1), labels, weight, bias.reshape(1, -1),
      out.reshape(-1, LANES))
    return pl.pallas_call(
        finish_kernel,
        out_shape=(
            jax.ShapeDtypeStruct(labels.shape, f32),
            jax.ShapeDtypeStruct((tables, hidden), f32),
            jax.ShapeDtypeStruct((1, hidden), f32),
        ),
        in_specs=[vmem] * 3,
        out_specs=(vmem,) * 3,
    )(logit, top, side)


def per_device(
    sample_ids, id_weights, dense_features, click_labels, table_shards, slot_table, top_weight, top_bias, out_weight
):
    micro, local_batch, columns = sample_ids.shape
    tables = slot_table.shape[0]
    slots = table_shards.shape[0]
    width = dense_features.shape[2]
    hidden = top_weight.shape[1]
    members = lax.axis_size("tab")
    groups = lax.axis_size("grp")
    samples = micro * local_batch
    count = samples * groups * members
    logit, grad_top, grad_bias = fused_step(
        count, groups, members, sample_ids, id_weights, dense_features.reshape(samples, width), table_shards,
        slot_table, click_labels, top_weight, top_bias, out_weight
    )
    return (logit, grad_top, grad_bias.reshape(hidden))


def solution(mesh):
    return jax.shard_map(
        per_device,
        mesh=mesh,
        in_specs=(
            P(None, ("grp", "tab"), None),
            P(None, ("grp", "tab"), None),
            P(None, ("grp", "tab"), None),
            P(None, ("grp", "tab")),
            P("tab", None, None),
            P(),
            P(),
            P(),
            P(),
        ),
        out_specs=(P(None, ("grp", "tab")), P(), P()),
        check_vma=False,
    )
```
